32 devices in a mesh: gx: 8 (over z, y), gy: 4 (over x, core).
Axes of the slice: x: 2, y: 2, z: 4, core: 2. Of those that a mesh axis runs over, the one named last changes fastest.
Arguments:
- table: float32 [4, 65536, 128], P(None, 'gx'), may hold values from -2.1 to 2.1
- lookup_owner: int32 [4, 8192, 16, 1], P(None, ('gx', 'gy')), may hold values from 0 to 7; in each aligned block of 4096 rows (0 to 4095, 4096 to 8191, ..., all dimensions but the last counted through in order) at most 1024 rows name the same one
- lookup_row: int32 [4, 8192, 16], P(None, ('gx', 'gy')), may hold values from 0 to 8191
- bag_length: int32 [4, 8192], P(None, ('gx', 'gy')), may hold values from 1 to 16
- top_in: bfloat16 [512, 8192], P(None, 'gy'), may hold values from -0.25 to 0.25
- top_bias: float32 [8192], P('gy'), may hold values from -3 to 3
- top_out: bfloat16 [8192, 1024], P('gy'), may hold values from -0.0625 to 0.0625
Outputs:
- scored: bfloat16 [8192, 1024], P(('gx', 'gy'))
The draws below stay inside these ranges and needn't reach their ends.
Inputs may be any that keep to these rules, and one draw needn't show every extreme that they name: `lookup_owner`: in every aligned block of 4096 entries (the lookups of one table from the samples of one device) no owner is named more than 1024 times; some blocks reach 1024.
All inputs are finite; a program needn't handle non-finite values.
Results may differ from the reference program's by a relative error of at most 0.0057.
Values may be sent and summed in bfloat16 or wider, within the bound.
A program may use at most 128 MiB of HBM per device.

```python
import math
import jax
import jax.numpy as jnp
import numpy as np
from jax import lax

EMB = 128
TABLES = 4
ROWS_DEV = 8192
SAMPLES_DEV = 256
BAG = 16
TOP_W = 8192
OUT_W = 1024
ROWS = 65536
BATCH = 8192
CAP = 1024
N_GX = 8


def set_ends(values, key, smallest, high):
    longest = values.shape.index(max(values.shape))
    spots = []
    for shift in (0, 1):
        where = [jax.random.randint(jax.random.fold_in(key, axis), (), 0, length) for axis, length in enumerate(values.shape)]
        where[longest] = (where[longest] + shift) % values.shape[longest]
        spots.append(tuple(where))
    return values.at[spots[0]].set(smallest).at[spots[1]].set(high)


def levels(stream_key, extent, cuts, low, top_value):
    level, own = 1.0, jax.random.fold_in(stream_key, 6)
    for dim, blocks in cuts:
        steps = jnp.exp(jax.random.uniform(jax.random.fold_in(own, dim), (blocks,), jnp.float32, low / len(cuts), top_value / len(cuts)))
        level = level * jnp.repeat(steps, extent[dim] // blocks).reshape([-1 if axis == dim else 1 for axis in range(len(extent))])
    return level


def rank_bounds(number_of, lean):
    portions = [(1 << 20) // math.isqrt(rank ** lean) + 1 for rank in range(1, number_of + 1)]
    width = 1 + sum(portions) // (1 << 30)
    return np.cumsum(np.array([max(1, weight // width) for weight in portions]))


def ranked_ids(stream_key, extent, number_of, skew):
    table = rank_bounds(number_of, skew)
    pick = jax.random.randint(jax.random.fold_in(stream_key, 1), extent, 0, int(table[number_of - 1]))
    rank = jnp.searchsorted(jnp.asarray(table, jnp.int32), pick, side="right")
    return jax.random.permutation(jax.random.fold_in(stream_key, 2), number_of)[rank].astype(jnp.int32)


def deal_out(stream_key, own, number, rows, number_of, top, most, slope):
    sequence = jax.random.permutation(stream_key, number_of)
    crowded, common = portions_of(number_of, rows * top, most, slope, True), portions_of(number_of, rows * top, most, slope, False)
    places = jnp.arange(number_of)

    def named(tallies, turn):
        used = int((tallies > 0).sum())
        fixed = max(1, used // 4)
        passed = fixed + (places - fixed + turn * (used - fixed)) % max(1, number_of - fixed)
        return jnp.zeros((number_of,), jnp.int32).at[sequence[jnp.where(places < fixed, places, passed)]].set(jnp.asarray(tallies, jnp.int32))

    tallies = jnp.where(number % 4 == 0, named(crowded, number // 4), named(common, number - number // 4 - 1))
    mixed = jax.random.permutation(jax.random.fold_in(own, 3), number_of)
    donor, receiver = mixed[0:number_of // 2 * 2:2], mixed[1:number_of // 2 * 2:2]
    margin = jnp.minimum(tallies[donor] - 1, most - tallies[receiver]) // 2
    margin = jnp.where((donor == sequence[0]) | (receiver == sequence[0]) | (tallies[receiver] == 0), 0, jnp.maximum(margin, 0))
    passed = jax.random.randint(jax.random.fold_in(own, 4), (number_of // 2,), 0, 1 << 20) % (margin + 1)
    tallies = tallies.at[donor].add(-passed).at[receiver].add(passed)
    labels = jnp.searchsorted(jnp.cumsum(tallies), jnp.arange(rows * top), side="right").astype(jnp.int32)
    table = labels.reshape(top, rows).T
    table = table[jax.random.permutation(jax.random.fold_in(own, 1), rows)]
    turn = jax.random.randint(jax.random.fold_in(own, 2), (rows, 1), 0, top)
    return jnp.take_along_axis(table, (jnp.arange(top)[None, :] + turn) % top, axis=1)


def portions_of(amount, total, reach, skew, full):
    weights = [(1 << 20) // math.isqrt(rank ** skew) + 1 for rank in range(1, amount + 1)]
    largest = reach if full else min(reach, max(-(-total // amount), total * weights[0] // sum(weights)))
    least = 1 if total - largest >= amount - 1 else 0
    counts, rest = [largest] + [least] * (amount - 1), total - largest - least * (amount - 1)
    while rest > 0:
        free = [i for i in range(1, amount) if counts[i] < largest] or [i for i in range(1, amount) if counts[i] < reach]
        pool, budget = sum([weights[i] for i in free]), rest
        for i in free:
            extra = min(reach - counts[i], max(1, budget * weights[i] // pool), rest)
            counts[i] = counts[i] + extra
            rest = rest - extra
    return np.array(counts)


def noise(rng, shape, deviation, bound, split=(), kind=jnp.bfloat16):
    drawn = jax.random.normal(rng, shape, jnp.float32) * deviation
    if len(split) > 0:
        drawn = levels(rng, shape, split, -0.22, 0.18) * drawn
    return jnp.clip(drawn, min=-bound, max=bound).astype(kind)


def setup_inputs(seed: int = 0) -> dict:
    seeds = jax.random.split(jax.random.key(seed), 8)
    table = noise(seeds[0], (TABLES, ROWS, EMB), 0.35, 2.1, ((1, 8),), jnp.float32)
    lookup_owner_keys = jax.random.split(jax.random.fold_in(seeds[1], 1), TABLES * BATCH * BAG // (SAMPLES_DEV * BAG))
    lookup_owner_turns = jax.random.permutation(jax.random.fold_in(seeds[1], 3), TABLES * BATCH * BAG // (SAMPLES_DEV * BAG))
    lookup_owner = jax.vmap(lambda own, number: deal_out(jax.random.fold_in(seeds[1], 2), own, number, SAMPLES_DEV * BAG, N_GX, 1, CAP, 1))(lookup_owner_keys, lookup_owner_turns).reshape((TABLES, BATCH, BAG, 1))
    lookup_row = set_ends(ranked_ids(seeds[2], (TABLES, BATCH, BAG), ROWS_DEV, 2), jax.random.fold_in(seeds[2], 3), 0, ROWS_DEV - 1).astype(jnp.int32)
    bag_length = set_ends(jax.random.randint(seeds[3], (TABLES, BATCH), 1, BAG + 1), jax.random.fold_in(seeds[3], 1), 1, BAG).astype(jnp.int32)
    top_in = noise(seeds[4], (TABLES * EMB, TOP_W), (TABLES * EMB) ** -0.5, 0.25, ((1, 4),))
    top_bias = noise(seeds[5], (TOP_W,), 0.5, 3.0, ((0, 4),), jnp.float32)
    top_out = noise(seeds[6], (TOP_W, OUT_W), TOP_W ** -0.5, 0.0625, ((0, 4),))
    return dict(table=table, lookup_owner=lookup_owner, lookup_row=lookup_row, bag_length=bag_length, top_in=top_in, top_bias=top_bias, top_out=top_out)


def pool_table(pieces):
    table_part, index_part, live_part = pieces
    fetched = jnp.take(table_part, index_part, axis=0)
    return jnp.sum(jnp.where(live_part[..., None], fetched, jnp.float32(0.0)), axis=1)


def reference(table, lookup_owner, lookup_row, bag_length, top_in, top_bias, top_out):
    row_index = (lookup_owner[..., 0] * ROWS_DEV + lookup_row).astype(jnp.int32)
    is_live = jnp.arange(BAG, dtype=jnp.int32)[None, None, :] < bag_length[:, :, None]
    pooled = lax.map(pool_table, (table, row_index, is_live))
    features = jnp.transpose(pooled, (1, 0, 2)).reshape(BATCH, TABLES * EMB).astype(jnp.bfloat16)
    blocks = features.reshape(N_GX, BATCH // N_GX, TABLES * EMB)

    def one_block(block):
        pre_act = jnp.dot(block, top_in, preferred_element_type=jnp.float32) + top_bias
        hidden_rows = jnp.maximum(pre_act, 0.0).astype(jnp.bfloat16)
        return jnp.dot(hidden_rows, top_out, preferred_element_type=jnp.float32).astype(jnp.bfloat16)

    scored = lax.map(one_block, blocks)
    return scored.reshape(BATCH, OUT_W)
```

```python
import functools
import jax
import jax.numpy as jnp
from jax import lax
from jax.experimental import pallas as pl
from jax.experimental.pallas import tpu as pltpu
from jax.sharding import PartitionSpec as P

BIG = 2**31 - 1
MESH = pl.DeviceIdType.MESH


def log2(n):
    return n.bit_length() - 1


def sort_kernel(rows_dev, owner_ref, row_ref, bag_ref, rows_ref, bags_ref, mine, outbox, held, send_sem, recv_sem):
    owners = held.shape[0]
    me = lax.axis_index("gx")
    barrier = pltpu.get_barrier_semaphore()
    for k in range(1, owners):
        pl.semaphore_signal(barrier, inc=1, device_id={"gx": lax.rem(me + k, owners)}, device_id_type=MESH)
    tables, bag_size, samples = owner_ref.shape
    owner = owner_ref[...]
    slot = lax.broadcasted_iota(jnp.int32, owner.shape, 1)
    sample = lax.broadcasted_iota(jnp.int32, owner.shape, 2)
    live = slot < bag_ref[...][:, None, :]
    key = jnp.where(live, (owner * samples + sample) * rows_dev + row_ref[...], BIG)
    count = bag_size * samples
    groups = count // 1024
    parts = []
    for t in range(tables):
        for c in range(samples // 128):
            for r in range(bag_size // 8):
                parts.append(key[t, r * 8 : r * 8 + 8, c * 128 : c * 128 + 128])
    lane = lax.broadcasted_iota(jnp.int32, (8, 128), 1)
    sub = lax.broadcasted_iota(jnp.int32, (8, 128), 0)
    place = sub * 128 + lane
    bits = log2(count)
    span = samples * rows_dev

    before = []
    for o in range(1, owners):
        for t in range(tables):
            tally = jnp.zeros((8, 128), jnp.int32)
            for g in range(groups):
                tally += (parts[t * groups + g] < o * span).astype(jnp.int32)
            before.append(jnp.sum(tally, axis=0, keepdims=True))
    before = jnp.sum(jnp.concatenate(before, axis=0), axis=1, keepdims=True)

    for k in range(1, bits + 1):
        for j in range(k - 1, -1, -1):
            d = 1 << j
            new = [None] * len(parts)
            for v in range(len(parts)):
                g = v % groups
                if d >= 1024:
                    gd = d // 1024
                    if g & gd:
                        continue
                    w = v + gd
                    low = jnp.minimum(parts[v], parts[w])
                    high = jnp.maximum(parts[v], parts[w])
                    up = ((g * 1024) >> k) & 1 == 0
                    new[v], new[w] = (low, high) if up else (high, low)
                    continue
                x = parts[v]
                if d < 128:
                    a, b = pltpu.roll(x, 128 - d, 1), pltpu.roll(x, d, 1)
                else:
                    s = d // 128
                    a, b = pltpu.roll(x, 8 - s, 0), pltpu.roll(x, s, 0)
                first = (place & d) == 0
                other = jnp.where(first, a, b)
                if (1 << k) >= 1024:
                    up = ((g * 1024) >> k) & 1 == 0
                    take_low = first if up else jnp.logical_not(first)
                else:
                    take_low = ((place >> k) ^ (place >> j)) & 1 == 0
                new[v] = jnp.where(take_low, jnp.minimum(x, other), jnp.maximum(x, other))
            parts = new
    wr = held.shape[1] // tables
    stride = mine.shape[0] // tables
    for t in range(tables):
        for g in range(groups):
            mine[t * stride + g * 8 : t * stride + g * 8 + 8, :] = parts[t * groups + g]
        mine[t * stride + groups * 8 : t * stride + stride, :] = jnp.full((stride - groups * 8, 128), BIG, jnp.int32)

    column = lax.broadcasted_iota(jnp.int32, (wr, 128), 1)
    for o in range(owners):
        for t in range(tables):
            if o == 0:
                x = mine[t * stride : t * stride + wr, :]
            else:
                off = before[(o - 1) * tables + t, 0]
                row = t * stride + (off >> 7)
                turn = off & 127
                a = pltpu.roll(mine[pl.ds(row, wr), :], 128 - turn, 1)
                b = pltpu.roll(mine[pl.ds(row + 1, wr), :], 128 - turn, 1)
                x = jnp.where(column < 128 - turn, a, b)
            x = x - o * span
            ours = jnp.logical_and(x >= 0, x < span)
            outbox[o, t * wr : t * wr + wr, :] = jnp.where(ours, x, span)

    pl.semaphore_wait(barrier, owners - 1)
    copies = []
    for k in range(1, owners):
        to = lax.rem(me + k, owners)
        copies.append(
            pltpu.make_async_remote_copy(
                src_ref=outbox.at[to],
                dst_ref=held.at[me],
                send_sem=send_sem.at[k],
                recv_sem=recv_sem.at[k],
                device_id={"gx": to},
                device_id_type=MESH,
            )
        )
        copies[-1].start()

    def split(source, get):
        for t in range(tables):
            x = get(pl.ds(t * wr, wr))
            rows_ref[source, t * wr : t * wr + wr, :] = (x & (rows_dev - 1)) + t * rows_dev
            bags_ref[source, t * wr : t * wr + wr, :] = x >> log2(rows_dev)

    split(me, lambda at: outbox[me, at, :])
    for k in range(1, owners):
        source = lax.rem(me - k + owners, owners)
        copies[k - 1].wait_recv()
        split(source, lambda at: held[source, at, :])
    for copy in copies:
        copy.wait_send()


def exchange_kernel(part_ref, top_in_ref, bias_ref, top_out_ref, out_ref, from_y, sum_y, from_z, feat, w_in, w_out, hid, near_out, near_in, far_out, w_send, far_in, wsem, ysem, yrec, zsem, zrec, gsem, grec, rsem, rrec, nsem, nrec, fsem, frec):
    owners, samples, width = part_ref.shape
    inner = from_y.shape[0] + 1
    outer = owners // inner
    chips = far_in.shape[0] + 1
    me, mine = lax.axis_index("gx"), lax.axis_index("gy")
    z, y = me // inner, lax.rem(me, inner)
    chip, core = mine // 2, lax.rem(mine, 2)
    partner = chip * 2 + 1 - core
    loads = [
        pltpu.make_async_copy(top_in_ref, w_in, wsem.at[0]),
        pltpu.make_async_copy(top_out_ref, w_out, wsem.at[1]),
    ]
    for load in loads:
        load.start()

    def gx_at(index):
        return {"gx": index}

    def gy_at(index):
        return {"gy": index}

    def remote(src, dst, send, recv, device):
        return pltpu.make_async_remote_copy(
            src_ref=src, dst_ref=dst, send_sem=send, recv_sem=recv, device_id=device, device_id_type=MESH
        )

    def y_at(d):
        return z * inner + lax.rem(y + d, inner)

    def z_at(d):
        return lax.rem(z + d, outer) * inner + y

    def chip_at(d):
        return lax.rem(chip + d, chips) * 2 + core

    peers = [gx_at(y_at(d)) for d in range(1, inner)]
    peers += [gx_at(z_at(d)) for d in range(1, outer)]
    peers += [gy_at(partner)] + [gy_at(chip_at(d)) for d in range(1, chips)]
    barrier = pltpu.get_barrier_semaphore()
    for peer in peers:
        pl.semaphore_signal(barrier, inc=1, device_id=peer, device_id_type=MESH)
    pl.semaphore_wait(barrier, len(peers))

    sends = []
    order = sorted(range(1, outer), key=lambda d: -min(d, outer - d)) + [0]
    y_copies = {}
    for dz in order:
        for d in range(1, inner):
            block = lax.rem(z + dz, outer)
            copy = remote(
                part_ref.at[block * inner + lax.rem(y + d, inner)],
                from_y.at[d - 1, dz],
                ysem.at[d - 1, dz],
                yrec.at[d - 1, dz],
                gx_at(y_at(d)),
            )
            copy.start()
            y_copies[dz, d] = copy
            sends.append(copy)
    step = 64
    z_copies = []
    for dz in order:
        block = lax.rem(z + dz, outer)
        for d in range(1, inner):
            y_copies[dz, d].wait_recv()

        @pl.loop(0, samples // step)
        def _(i):
            rows = pl.ds(pl.multiple_of(i * step, step), step)
            total = part_ref[block * inner + y, rows, :].astype(jnp.float32)
            for d in range(1, inner):
                total += from_y[d - 1, dz, rows, :].astype(jnp.float32)
            sum_y[dz, rows, :] = total.astype(sum_y.dtype)

        if dz:
            copy = remote(sum_y.at[dz], from_z.at[dz - 1], zsem.at[dz - 1], zrec.at[dz - 1], gx_at(z_at(dz)))
            copy.start()
            z_copies.append(copy)
    for copy in z_copies:
        copy.wait_recv()

    @pl.loop(0, samples // step)
    def _(i):
        rows = pl.ds(pl.multiple_of(i * step, step), step)
        total = sum_y[0, rows, :].astype(jnp.float32)
        for d in range(1, outer):
            total += from_z[d - 1, rows, :].astype(jnp.float32)
        feat[0, rows, :] = total.astype(feat.dtype)

    far = []
    for d in range(1, chips):
        copy = remote(feat.at[0], feat.at[2 * (chips - d)], gsem.at[d], grec.at[chips - d], gy_at(chip_at(d)))
        copy.start()
        far.append(copy)
    near = [remote(feat.at[0], feat.at[1], rsem.at[0], rrec.at[0], gy_at(partner))]
    near[0].start()
    for load in loads:
        load.wait()
    tile = 512
    hidden, outs = w_in.shape[1], w_out.shape[1]

    def scores(index, put):
        @pl.loop(0, hidden // tile)
        def _(i):
            cols = pl.ds(pl.multiple_of(i * tile, tile), tile)
            pre = jnp.dot(feat[index], w_in[:, cols], preferred_element_type=jnp.float32) + bias_ref[:, cols]
            hid[:, cols] = jnp.maximum(pre, 0.0).astype(hid.dtype)

        @pl.loop(0, outs // tile)
        def _(i):
            cols = pl.ds(pl.multiple_of(i * tile, tile), tile)
            put(cols, jnp.dot(hid[...], w_out[:, cols], preferred_element_type=jnp.float32))

    def to_partner(d):
        def put(cols, value):
            near_out[d, :, cols] = value.astype(near_out.dtype)

        scores(2 * d + 1, put)
        copy = remote(near_out.at[d], near_in.at[d], nsem.at[d], nrec.at[d], gy_at(partner))
        copy.start()
        return copy

    def kept(d):
        def put(cols, value):
            far_out[d, :, cols] = value

        scores(2 * d, put)

    last = []
    kept(0)
    near[0].wait_recv()
    last.append(to_partner(0))
    for d in range(1, chips):
        far[chips - 1 - d].wait_recv()
        copy = remote(feat.at[2 * d], feat.at[2 * d + 1], rsem.at[d], rrec.at[d], gy_at(partner))
        copy.start()
        near.append(copy)
        kept(d)
        copy.wait_recv()
        last.append(to_partner(d))
    far_copies = []
    for d in range(1, chips):
        last[d].wait_recv()

        @pl.loop(0, samples // step)
        def _(i):
            rows = pl.ds(pl.multiple_of(i * step, step), step)
            total = far_out[d, rows, :] + near_in[d, rows, :].astype(jnp.float32)
            w_send[d - 1, rows, :] = total.astype(w_send.dtype)

        copy = remote(w_send.at[d - 1], far_in.at[d - 1], fsem.at[d - 1], frec.at[d - 1], gy_at(chip_at(d)))
        copy.start()
        far_copies.append(copy)
    last[0].wait_recv()
    for copy in far_copies:
        copy.wait_recv()

    @pl.loop(0, samples // step)
    def _(i):
        rows = pl.ds(pl.multiple_of(i * step, step), step)
        total = far_out[0, rows, :] + near_in[0, rows, :].astype(jnp.float32)
        for d in range(1, chips):
            total += far_in[d - 1, rows, :].astype(jnp.float32)
        out_ref[rows, :] = total.astype(out_ref.dtype)

    for copy in sends + z_copies + far + near + last + far_copies:
        copy.wait_send()


def pool_kernel(rows_hbm, bags_ref, table_ref, out_ref, tab, stage, acc, rows, lives, tsem, ksem):
    tables, rows_dev, emb = table_ref.shape
    sources, samples, _ = out_ref.shape
    wr = bags_ref.shape[1] // tables
    window = wr * 128
    loads = [
        pltpu.make_async_copy(table_ref.at[t], tab.at[pl.ds(t * rows_dev, rows_dev)], tsem.at[t])
        for t in range(tables)
    ]
    keys = pltpu.make_async_copy(rows_hbm, rows, ksem)
    keys.start()
    for load in loads:
        load.start()
    tallies = []
    for s in range(sources):
        for t in range(tables):
            live = (bags_ref[s, t * wr : t * wr + wr, :] < samples).astype(jnp.int32)
            tallies.append(jnp.sum(live, axis=0, keepdims=True))
    tallies = jnp.sum(jnp.concatenate(tallies, axis=0), axis=1, keepdims=True)
    for i in range(sources * tables):
        lives[i] = tallies[i, 0]
    stage[...] = jnp.zeros_like(stage)
    place = lax.broadcasted_iota(jnp.int32, (samples, 128), 0)
    keys.wait()

    def staged(side):
        return stage[pl.ds(pl.multiple_of(side * 128, 128), 128), :].astype(jnp.bfloat16)

    def add(source, t, j, held):
        row = bags_ref[source, pl.ds(t * wr + j, 1), :]
        pick = jnp.where(place == row, 1.0, 0.0).astype(jnp.bfloat16)
        more = jnp.dot(pick, held, preferred_element_type=jnp.float32)
        total = jnp.where(j == 0, 0.0, acc[...]) + more
        acc[...] = total
        out_ref[source, :, pl.ds(pl.multiple_of(t * emb, emb), emb)] = total.astype(out_ref.dtype)

    def item(source, t, carry):
        blocks = jnp.maximum((lives[source * tables + t] + 127) // 128, 1)

        def block(j, carry):
            side, old_source, old_t, old_j = carry
            base = (source * tables + t) * window + j * 128
            held = staged(1 - side)
            to = side * 128
            for u in range(128):
                stage[pl.ds(to + u, 1), :] = tab[pl.ds(rows[base + u], 1), :]
            add(old_source, old_t, old_j, held)
            return 1 - side, source, t, j

        return lax.fori_loop(0, blocks, block, carry)

    carry = (jnp.int32(0), jnp.int32(0), jnp.int32(0), jnp.int32(0))
    for t in range(tables):
        loads[t].wait()
        carry = lax.fori_loop(0, sources, lambda s, c: item(s, jnp.int32(t), c), carry)
    side, source, t, j = carry
    add(source, t, j, staged(1 - side))


def local(table, lookup_owner, lookup_row, bag_length, top_in, top_bias, top_out):
    owners = lax.axis_size("gx")
    me = lax.axis_index("gx")
    tables, samples, bag_size = lookup_row.shape
    rows_dev = table.shape[1]
    emb = table.shape[2]
    count = samples * bag_size
    cap = 2 * count // owners
    wr = -(-cap // 128)
    vmem = pl.BlockSpec(memory_space=pltpu.VMEM)
    anywhere = pl.BlockSpec(memory_space=pl.ANY)

    windows = jax.ShapeDtypeStruct((owners, tables * wr, 128), jnp.int32)
    rows, bags = pl.pallas_call(
        functools.partial(sort_kernel, rows_dev),
        out_shape=(windows, windows),
        scratch_shapes=[
            pltpu.VMEM((tables * (count // 128 + 16), 128), jnp.int32),
            pltpu.VMEM((owners, tables * wr, 128), jnp.int32),
            pltpu.VMEM((owners, tables * wr, 128), jnp.int32),
            pltpu.SemaphoreType.DMA((owners,)),
            pltpu.SemaphoreType.DMA((owners,)),
        ],
        compiler_params=pltpu.CompilerParams(collective_id=0, has_side_effects=True),
        name="sort_keys",
    )(
        jnp.transpose(lookup_owner[..., 0], (0, 2, 1)),
        jnp.transpose(lookup_row, (0, 2, 1)),
        bag_length,
    )
    partial = pl.pallas_call(
        pool_kernel,
        out_shape=jax.ShapeDtypeStruct((owners, samples, tables * emb), jnp.bfloat16),
        in_specs=[anywhere, vmem, anywhere],
        out_specs=vmem,
        scratch_shapes=[
            pltpu.VMEM((tables * rows_dev, emb), jnp.float32),
            pltpu.VMEM((256, emb), jnp.float32),
            pltpu.VMEM((samples, emb), jnp.float32),
            pltpu.SMEM((owners * tables * wr * 128,), jnp.int32),
            pltpu.SMEM((owners * tables,), jnp.int32),
            pltpu.SemaphoreType.DMA((tables,)),
            pltpu.SemaphoreType.DMA,
        ],
        name="pool",
    )(rows.reshape(-1), bags, table)
    inner = max(1, owners // 4)
    outer = owners // inner
    chips = lax.axis_size("gy") // 2
    width = tables * emb
    hidden, outs = top_out.shape
    bf16, dma = jnp.bfloat16, pltpu.SemaphoreType.DMA
    return pl.pallas_call(
        exchange_kernel,
        out_shape=jax.ShapeDtypeStruct((samples, outs), bf16),
        in_specs=[vmem, pl.BlockSpec(memory_space=pl.ANY), vmem, pl.BlockSpec(memory_space=pl.ANY)],
        out_specs=vmem,
        scratch_shapes=[
            pltpu.VMEM((inner - 1, outer, samples, width), bf16),
            pltpu.VMEM((outer, samples, width), bf16),
            pltpu.VMEM((outer - 1, samples, width), bf16),
            pltpu.VMEM((2 * chips, samples, width), bf16),
            pltpu.VMEM((width, hidden), bf16),
            pltpu.VMEM((hidden, outs), bf16),
            pltpu.VMEM((samples, hidden), bf16),
            pltpu.VMEM((chips, samples, outs), bf16),
            pltpu.VMEM((chips, samples, outs), bf16),
            pltpu.VMEM((chips, samples, outs), jnp.float32),
            pltpu.VMEM((chips - 1, samples, outs), bf16),
            pltpu.VMEM((chips - 1, samples, outs), bf16),
            dma((2,)),
            dma((inner - 1, outer)),
            dma((inner - 1, outer)),
            dma((outer - 1,)),
            dma((outer - 1,)),
            dma((chips,)),
            dma((chips,)),
            dma((chips,)),
            dma((chips,)),
            dma((chips,)),
            dma((chips,)),
            dma((chips - 1,)),
            dma((chips - 1,)),
        ],
        compiler_params=pltpu.CompilerParams(
            collective_id=1, has_side_effects=True, vmem_limit_bytes=50 * 2**20
        ),
        name="exchange",
    )(partial, top_in, top_bias[None, :], top_out)


def solution(mesh):
    return jax.shard_map(
        local,
        mesh=mesh,
        in_specs=(
            P(None, "gx", None),
            P(None, ("gx", "gy"), None, None),
            P(None, ("gx", "gy"), None),
            P(None, ("gx", "gy")),
            P(None, "gy"),
            P("gy"),
            P("gy", None),
        ),
        out_specs=P(("gx", "gy"), None),
        check_vma=False,
    )
```

```python
import functools
import jax
import jax.numpy as jnp
from jax import lax
from jax.experimental import pallas as pl
from jax.experimental.pallas import tpu as pltpu
from jax.sharding import PartitionSpec as P

BIG = 2**31 - 1
MESH = pl.DeviceIdType.MESH


def log2(n):
    return n.bit_length() - 1


def sort_kernel(rows_dev, owner_ref, row_ref, bag_ref, rows_ref, bags_ref, mine, outbox, held, send_sem, recv_sem):
    owners = held.shape[0]
    me = lax.axis_index("gx")
    barrier = pltpu.get_barrier_semaphore()
    for k in range(1, owners):
        pl.semaphore_signal(barrier, inc=1, device_id={"gx": lax.rem(me + k, owners)}, device_id_type=MESH)
    tables, bag_size, samples = owner_ref.shape
    owner = owner_ref[...]
    slot = lax.broadcasted_iota(jnp.int32, owner.shape, 1)
    sample = lax.broadcasted_iota(jnp.int32, owner.shape, 2)
    live = slot < bag_ref[...][:, None, :]
    key = jnp.where(live, (owner * samples + sample) * rows_dev + row_ref[...], BIG)
    count = bag_size * samples
    groups = count // 1024
    parts = []
    for t in range(tables):
        for c in range(samples // 128):
            for r in range(bag_size // 8):
                parts.append(key[t, r * 8 : r * 8 + 8, c * 128 : c * 128 + 128])
    lane = lax.broadcasted_iota(jnp.int32, (8, 128), 1)
    sub = lax.broadcasted_iota(jnp.int32, (8, 128), 0)
    place = lane * 8 + sub
    bits = log2(count)
    span = samples * rows_dev

    before = []
    for o in range(1, owners):
        for t in range(tables):
            tally = jnp.zeros((8, 128), jnp.int32)
            for g in range(groups):
                tally += (parts[t * groups + g] < o * span).astype(jnp.int32)
            before.append(jnp.sum(tally, axis=0, keepdims=True))
    before = jnp.sum(jnp.concatenate(before, axis=0), axis=1, keepdims=True)

    for k in range(1, bits + 1):
        for j in range(k - 1, -1, -1):
            d = 1 << j
            new = [None] * len(parts)
            for v in range(len(parts)):
                g = v % groups
                if d >= 1024:
                    gd = d // 1024
                    if g & gd:
                        continue
                    w = v + gd
                    low = jnp.minimum(parts[v], parts[w])
                    high = jnp.maximum(parts[v], parts[w])
                    up = ((g * 1024) >> k) & 1 == 0
                    new[v], new[w] = (low, high) if up else (high, low)
                    continue
                x = parts[v]
                if d < 8:
                    a, b = pltpu.roll(x, 8 - d, 0), pltpu.roll(x, d, 0)
                else:
                    s = d // 8
                    a, b = pltpu.roll(x, 128 - s, 1), pltpu.roll(x, s, 1)
                first = (place & d) == 0
                other = jnp.where(first, a, b)
                if (1 << k) >= 1024:
                    up = ((g * 1024) >> k) & 1 == 0
                    take_low = first if up else jnp.logical_not(first)
                else:
                    take_low = ((place >> k) ^ (place >> j)) & 1 == 0
                new[v] = jnp.where(take_low, jnp.minimum(x, other), jnp.maximum(x, other))
            parts = new
    stride = mine.shape[0] // tables
    for t in range(tables):
        for g in range(stride // 8):
            at = t * stride + g * 8
            mine[at : at + 8, :] = parts[t * groups + g] if g < groups else jnp.full((8, 128), BIG, jnp.int32)

    for o in range(owners):
        for t in range(tables):
            if o == 0:
                x = mine[t * stride : t * stride + 8, :]
            else:
                off = before[(o - 1) * tables + t, 0]
                low = off & 7

                def columns(first):
                    at = t * stride + ((first >> 7) << 3)
                    left = 128 - (first & 127)
                    turn = left & 127
                    p = pltpu.roll(mine[pl.ds(at, 8), :], turn, 1)
                    q = pltpu.roll(mine[pl.ds(at + 8, 8), :], turn, 1)
                    return pltpu.roll(jnp.where(lane < left, p, q), (8 - low) & 7, 0)

                x = jnp.where(sub < 8 - low, columns(off >> 3), columns((off >> 3) + 1))
            x = x - o * span
            ours = jnp.logical_and(x >= 0, x < span)
            outbox[o, t * 8 : t * 8 + 8, :] = jnp.where(ours, x, span)

    pl.semaphore_wait(barrier, owners - 1)
    copies = []
    for k in range(1, owners):
        to = lax.rem(me + k, owners)
        copies.append(
            pltpu.make_async_remote_copy(
                src_ref=outbox.at[to],
                dst_ref=held.at[me],
                send_sem=send_sem.at[k],
                recv_sem=recv_sem.at[k],
                device_id={"gx": to},
                device_id_type=MESH,
            )
        )
        copies[-1].start()

    def split(source, get):
        for t in range(tables):
            x = get(pl.ds(t * 8, 8))
            rows_ref[:, pl.ds(source * tables + t, 1), :] = ((x & (rows_dev - 1)) + t * rows_dev)[:, None, :]
            bags_ref[source, t * 8 : t * 8 + 8, :] = x >> log2(rows_dev)

    split(me, lambda at: outbox[me, at, :])
    for k in range(1, owners):
        source = lax.rem(me - k + owners, owners)
        copies[k - 1].wait_recv()
        split(source, lambda at: held[source, at, :])
    for copy in copies:
        copy.wait_send()


def exchange_kernel(part_ref, top_in_ref, bias_ref, top_out_ref, out_ref, from_y, sum_y, from_z, feat, w_in, w_out, hid, near_out, near_in, far_out, w_send, far_in, wsem, ysem, yrec, zsem, zrec, gsem, grec, rsem, rrec, nsem, nrec, fsem, frec):
    owners, samples, width = part_ref.shape
    inner = from_y.shape[0] + 1
    outer = owners // inner
    chips = far_in.shape[0] + 1
    me, mine = lax.axis_index("gx"), lax.axis_index("gy")
    z, y = me // inner, lax.rem(me, inner)
    chip, core = mine // 2, lax.rem(mine, 2)
    partner = chip * 2 + 1 - core
    loads = [
        pltpu.make_async_copy(top_in_ref, w_in, wsem.at[0]),
        pltpu.make_async_copy(top_out_ref, w_out, wsem.at[1]),
    ]
    for load in loads:
        load.start()

    def gx_at(index):
        return {"gx": index}

    def gy_at(index):
        return {"gy": index}

    def remote(src, dst, send, recv, device):
        return pltpu.make_async_remote_copy(
            src_ref=src, dst_ref=dst, send_sem=send, recv_sem=recv, device_id=device, device_id_type=MESH
        )

    def y_at(d):
        return z * inner + lax.rem(y + d, inner)

    def z_at(d):
        return lax.rem(z + d, outer) * inner + y

    def chip_at(d):
        return lax.rem(chip + d, chips) * 2 + core

    peers = [gx_at(y_at(d)) for d in range(1, inner)]
    peers += [gx_at(z_at(d)) for d in range(1, outer)]
    peers += [gy_at(partner)] + [gy_at(chip_at(d)) for d in range(1, chips)]
    barrier = pltpu.get_barrier_semaphore()
    for peer in peers:
        pl.semaphore_signal(barrier, inc=1, device_id=peer, device_id_type=MESH)
    pl.semaphore_wait(barrier, len(peers))

    sends = []
    order = sorted(range(1, outer), key=lambda d: -min(d, outer - d)) + [0]
    y_copies = {}
    for dz in order:
        for d in range(1, inner):
            block = lax.rem(z + dz, outer)
            copy = remote(
                part_ref.at[block * inner + lax.rem(y + d, inner)],
                from_y.at[d - 1, dz],
                ysem.at[d - 1, dz],
                yrec.at[d - 1, dz],
                gx_at(y_at(d)),
            )
            copy.start()
            y_copies[dz, d] = copy
            sends.append(copy)
    step = 64
    z_copies = []
    for dz in order:
        block = lax.rem(z + dz, outer)
        for d in range(1, inner):
            y_copies[dz, d].wait_recv()

        @pl.loop(0, samples // step)
        def _(i):
            rows = pl.ds(pl.multiple_of(i * step, step), step)
            total = part_ref[block * inner + y, rows, :].astype(jnp.float32)
            for d in range(1, inner):
                total += from_y[d - 1, dz, rows, :].astype(jnp.float32)
            sum_y[dz, rows, :] = total.astype(sum_y.dtype)

        if dz:
            copy = remote(sum_y.at[dz], from_z.at[dz - 1], zsem.at[dz - 1], zrec.at[dz - 1], gx_at(z_at(dz)))
            copy.start()
            z_copies.append(copy)
    for copy in z_copies:
        copy.wait_recv()

    @pl.loop(0, samples // step)
    def _(i):
        rows = pl.ds(pl.multiple_of(i * step, step), step)
        total = sum_y[0, rows, :].astype(jnp.float32)
        for d in range(1, outer):
            total += from_z[d - 1, rows, :].astype(jnp.float32)
        feat[0, rows, :] = total.astype(feat.dtype)

    far = []
    for d in range(1, chips):
        copy = remote(feat.at[0], feat.at[2 * (chips - d)], gsem.at[d], grec.at[chips - d], gy_at(chip_at(d)))
        copy.start()
        far.append(copy)
    near = [remote(feat.at[0], feat.at[1], rsem.at[0], rrec.at[0], gy_at(partner))]
    near[0].start()
    for load in loads:
        load.wait()
    tile = 512
    hidden, outs = w_in.shape[1], w_out.shape[1]

    def scores(index, put):
        @pl.loop(0, hidden // tile)
        def _(i):
            cols = pl.ds(pl.multiple_of(i * tile, tile), tile)
            pre = jnp.dot(feat[index], w_in[:, cols], preferred_element_type=jnp.float32) + bias_ref[:, cols]
            hid[:, cols] = jnp.maximum(pre, 0.0).astype(hid.dtype)

        @pl.loop(0, outs // tile)
        def _(i):
            cols = pl.ds(pl.multiple_of(i * tile, tile), tile)
            put(cols, jnp.dot(hid[...], w_out[:, cols], preferred_element_type=jnp.float32))

    def to_partner(d):
        def put(cols, value):
            near_out[d, :, cols] = value.astype(near_out.dtype)

        scores(2 * d + 1, put)
        copy = remote(near_out.at[d], near_in.at[d], nsem.at[d], nrec.at[d], gy_at(partner))
        copy.start()
        return copy

    def kept(d):
        def put(cols, value):
            far_out[d, :, cols] = value

        scores(2 * d, put)

    last = []
    kept(0)
    near[0].wait_recv()
    last.append(to_partner(0))
    for d in range(1, chips):
        far[chips - 1 - d].wait_recv()
        copy = remote(feat.at[2 * d], feat.at[2 * d + 1], rsem.at[d], rrec.at[d], gy_at(partner))
        copy.start()
        near.append(copy)
        kept(d)
        copy.wait_recv()
        last.append(to_partner(d))
    far_copies = []
    for d in range(1, chips):
        last[d].wait_recv()

        @pl.loop(0, samples // step)
        def _(i):
            rows = pl.ds(pl.multiple_of(i * step, step), step)
            total = far_out[d, rows, :] + near_in[d, rows, :].astype(jnp.float32)
            w_send[d - 1, rows, :] = total.astype(w_send.dtype)

        copy = remote(w_send.at[d - 1], far_in.at[d - 1], fsem.at[d - 1], frec.at[d - 1], gy_at(chip_at(d)))
        copy.start()
        far_copies.append(copy)
    last[0].wait_recv()
    for copy in far_copies:
        copy.wait_recv()

    @pl.loop(0, samples // step)
    def _(i):
        rows = pl.ds(pl.multiple_of(i * step, step), step)
        total = far_out[0, rows, :] + near_in[0, rows, :].astype(jnp.float32)
        for d in range(1, chips):
            total += far_in[d - 1, rows, :].astype(jnp.float32)
        out_ref[rows, :] = total.astype(out_ref.dtype)

    for copy in sends + z_copies + far + near + last + far_copies:
        copy.wait_send()


def pool_kernel(rows_hbm, bags_ref, table_ref, out_ref, tab, stage, rows, lives, tsem, ksem):
    tables, rows_dev, emb = table_ref.shape
    sources, samples, _ = out_ref.shape
    items = sources * tables
    loads = [
        pltpu.make_async_copy(table_ref.at[t], tab.at[pl.ds(t * rows_dev, rows_dev)], tsem.at[t])
        for t in range(tables)
    ]
    keys = [
        pltpu.make_async_copy(rows_hbm.at[pl.ds(u * items * 128, items * 128)], rows[u], ksem.at[u])
        for u in range(8)
    ]
    for copy in keys + loads:
        copy.start()
    tallies = []
    for i in range(items):
        live = (bags_ref[i // tables, i % tables * 8 : i % tables * 8 + 8, :] < samples).astype(jnp.int32)
        tallies.append(jnp.sum(live, axis=0, keepdims=True))
    tallies = jnp.sum(jnp.concatenate(tallies, axis=0), axis=1, keepdims=True)
    for i in range(items):
        lives[i] = tallies[i, 0]
    stage[...] = jnp.zeros_like(stage)
    place = lax.broadcasted_iota(jnp.int32, (samples, 128), 0)
    for copy in keys:
        copy.wait()

    for t in range(tables):
        loads[t].wait()

        @pl.loop(0, sources)
        def _(s):
            item = s * tables + t

            @pl.loop(0, (lives[item] + 63) // 64)
            def _(i):
                for k in range(8):
                    key = item * 128 + i * 8 + k
                    for u in range(8):
                        stage[pl.ds(s * 1024 + i * 8 + u * 128 + k, 1), :] = tab[pl.ds(rows[u][key], 1), :]

        @pl.loop(0, sources // 4)
        def _(i):
            for k in range(4):
                s = i * 4 + k
                picks = []
                for u in range(8):
                    bag = bags_ref[s, t * 8 + u : t * 8 + u + 1, :]
                    picks.append(jnp.where(place == bag, 1.0, 0.0).astype(jnp.bfloat16))
                held = stage[pl.ds(pl.multiple_of(s * 1024, 1024), 1024), :].astype(jnp.bfloat16)
                total = jnp.dot(jnp.concatenate(picks, axis=1), held, preferred_element_type=jnp.float32)
                out_ref[s, :, t * emb : (t + 1) * emb] = total.astype(out_ref.dtype)


def local(table, lookup_owner, lookup_row, bag_length, top_in, top_bias, top_out):
    owners = lax.axis_size("gx")
    me = lax.axis_index("gx")
    tables, samples, bag_size = lookup_row.shape
    rows_dev = table.shape[1]
    emb = table.shape[2]
    count = samples * bag_size
    assert 2 * count // owners <= 1024
    vmem = pl.BlockSpec(memory_space=pltpu.VMEM)
    anywhere = pl.BlockSpec(memory_space=pl.ANY)

    items = owners * tables
    windows = pltpu.VMEM((owners, tables * 8, 128), jnp.int32)
    rows, bags = pl.pallas_call(
        functools.partial(sort_kernel, rows_dev),
        out_shape=(
            jax.ShapeDtypeStruct((8, items, 128), jnp.int32),
            jax.ShapeDtypeStruct((owners, tables * 8, 128), jnp.int32),
        ),
        scratch_shapes=[
            pltpu.VMEM((tables * (count // 128 + 16), 128), jnp.int32),
            windows,
            windows,
            pltpu.SemaphoreType.DMA((owners,)),
            pltpu.SemaphoreType.DMA((owners,)),
        ],
        compiler_params=pltpu.CompilerParams(collective_id=0, has_side_effects=True),
        name="sort_keys",
    )(
        jnp.transpose(lookup_owner[..., 0], (0, 2, 1)),
        jnp.transpose(lookup_row, (0, 2, 1)),
        bag_length,
    )
    partial = pl.pallas_call(
        pool_kernel,
        out_shape=jax.ShapeDtypeStruct((owners, samples, tables * emb), jnp.bfloat16),
        in_specs=[anywhere, vmem, anywhere],
        out_specs=vmem,
        scratch_shapes=[
            pltpu.VMEM((tables * rows_dev, emb), jnp.float32),
            pltpu.VMEM((owners * 1024, emb), jnp.float32),
            [pltpu.SMEM((items * 128,), jnp.int32) for _ in range(8)],
            pltpu.SMEM((items,), jnp.int32),
            pltpu.SemaphoreType.DMA((tables,)),
            pltpu.SemaphoreType.DMA((8,)),
        ],
        name="pool",
    )(rows.reshape(-1), bags, table)
    inner = max(1, owners // 4)
    outer = owners // inner
    chips = lax.axis_size("gy") // 2
    width = tables * emb
    hidden, outs = top_out.shape
    bf16, dma = jnp.bfloat16, pltpu.SemaphoreType.DMA
    return pl.pallas_call(
        exchange_kernel,
        out_shape=jax.ShapeDtypeStruct((samples, outs), bf16),
        in_specs=[vmem, pl.BlockSpec(memory_space=pl.ANY), vmem, pl.BlockSpec(memory_space=pl.ANY)],
        out_specs=vmem,
        scratch_shapes=[
            pltpu.VMEM((inner - 1, outer, samples, width), bf16),
            pltpu.VMEM((outer, samples, width), bf16),
            pltpu.VMEM((outer - 1, samples, width), bf16),
            pltpu.VMEM((2 * chips, samples, width), bf16),
            pltpu.VMEM((width, hidden), bf16),
            pltpu.VMEM((hidden, outs), bf16),
            pltpu.VMEM((samples, hidden), bf16),
            pltpu.VMEM((chips, samples, outs), bf16),
            pltpu.VMEM((chips, samples, outs), bf16),
            pltpu.VMEM((chips, samples, outs), jnp.float32),
            pltpu.VMEM((chips - 1, samples, outs), bf16),
            pltpu.VMEM((chips - 1, samples, outs), bf16),
            dma((2,)),
            dma((inner - 1, outer)),
            dma((inner - 1, outer)),
            dma((outer - 1,)),
            dma((outer - 1,)),
            dma((chips,)),
            dma((chips,)),
            dma((chips,)),
            dma((chips,)),
            dma((chips,)),
            dma((chips,)),
            dma((chips - 1,)),
            dma((chips - 1,)),
        ],
        compiler_params=pltpu.CompilerParams(
            collective_id=1, has_side_effects=True, vmem_limit_bytes=50 * 2**20
        ),
        name="exchange",
    )(partial, top_in, top_bias[None, :], top_out)


def solution(mesh):
    return jax.shard_map(
        local,
        mesh=mesh,
        in_specs=(
            P(None, "gx", None),
            P(None, ("gx", "gy"), None, None),
            P(None, ("gx", "gy"), None),
            P(None, ("gx", "gy")),
            P(None, "gy"),
            P("gy"),
            P("gy", None),
        ),
        out_specs=P(("gx", "gy"), None),
        check_vma=False,
    )
```

```python
import jax
import jax.numpy as jnp
from jax import lax
from jax.experimental import pallas as pl
from jax.experimental.pallas import tpu as pltpu
from jax.sharding import PartitionSpec as P

CHUNKS = 4
BIG = 2**31 - 1
MESH = pl.DeviceIdType.MESH


def log2(n):
    return n.bit_length() - 1


def bags_kernel(owner_ref, row_ref, bag_ref, table_ref, top_in_ref, bias_ref, top_out_ref, out_ref, mine, outbox, held, row_list, bag_list, rows, tab, stage, part_y, part_own, from_y, sum_y, from_z, feat, w_in, w_out, hid, kept, give, take, x_send, x_take, tsem, wsem, rsem, ksend, krec, ysend, yrec, zsend, zrec, gsend, grec, nsend, nrec, bsend, brec, fsend, frec):
    owners = held.shape[0]
    inner, outer = from_y.shape[0] + 1, sum_y.shape[0] + 1
    chips, chunks, rows_pair, width = feat.shape
    step = rows_pair // 2
    rows_dev = table_ref.shape[1]
    emb = table_ref.shape[2]
    me, mine_y = lax.axis_index("gx"), lax.axis_index("gy")
    z, y = me // inner, lax.rem(me, inner)
    chip, core = mine_y // 2, lax.rem(mine_y, 2)
    partner = {"gy": chip * 2 + 1 - core}

    def remote(src, dst, send, recv, device):
        return pltpu.make_async_remote_copy(
            src_ref=src, dst_ref=dst, send_sem=send, recv_sem=recv, device_id=device, device_id_type=MESH
        )

    def gx_at(dz, d):
        return {"gx": lax.rem(z + dz, outer) * inner + lax.rem(y + d, inner)}

    def chip_at(d):
        return {"gy": lax.rem(chip + d, chips) * 2 + core}

    barrier = pltpu.get_barrier_semaphore()
    peers = [gx_at(dz, d) for dz in range(outer) for d in range(inner) if dz or d]
    peers += [partner] + [chip_at(d) for d in range(1, chips)]
    for peer in peers:
        pl.semaphore_signal(barrier, inc=1, device_id=peer, device_id_type=MESH)
    tables_in = [
        pltpu.make_async_copy(table_ref.at[t], tab.at[pl.ds(t * rows_dev, rows_dev)], tsem.at[t])
        for t in range(table_ref.shape[0])
    ]
    weights_in = [
        pltpu.make_async_copy(top_in_ref, w_in, wsem.at[0]),
        pltpu.make_async_copy(top_out_ref, w_out, wsem.at[1]),
    ]
    for load in tables_in + weights_in:
        load.start()

    tables, bag_size, samples = owner_ref.shape
    owner = owner_ref[...]
    slot = lax.broadcasted_iota(jnp.int32, owner.shape, 1)
    sample = lax.broadcasted_iota(jnp.int32, owner.shape, 2)
    live = slot < bag_ref[...][:, None, :]
    key = jnp.where(live, (owner * samples + sample) * rows_dev + row_ref[...], BIG)
    count = bag_size * samples
    groups = count // 1024
    parts = []
    for t in range(tables):
        for c in range(samples // 128):
            for r in range(bag_size // 8):
                parts.append(key[t, r * 8 : r * 8 + 8, c * 128 : c * 128 + 128])
    lane = lax.broadcasted_iota(jnp.int32, (8, 128), 1)
    sub = lax.broadcasted_iota(jnp.int32, (8, 128), 0)
    place = lane * 8 + sub
    bits = log2(count)
    span = samples * rows_dev

    before = []
    for o in range(1, owners):
        for t in range(tables):
            tally = jnp.zeros((8, 128), jnp.int32)
            for g in range(groups):
                tally += (parts[t * groups + g] < o * span).astype(jnp.int32)
            before.append(jnp.sum(tally, axis=0, keepdims=True))
    before = jnp.sum(jnp.concatenate(before, axis=0), axis=1, keepdims=True)

    for k in range(1, bits + 1):
        for j in range(k - 1, -1, -1):
            d = 1 << j
            new = [None] * len(parts)
            for v in range(len(parts)):
                g = v % groups
                if d >= 1024:
                    gd = d // 1024
                    if g & gd:
                        continue
                    w = v + gd
                    low = jnp.minimum(parts[v], parts[w])
                    high = jnp.maximum(parts[v], parts[w])
                    up = ((g * 1024) >> k) & 1 == 0
                    new[v], new[w] = (low, high) if up else (high, low)
                    continue
                x = parts[v]
                if d < 8:
                    a, b = pltpu.roll(x, 8 - d, 0), pltpu.roll(x, d, 0)
                else:
                    s = d // 8
                    a, b = pltpu.roll(x, 128 - s, 1), pltpu.roll(x, s, 1)
                first = (place & d) == 0
                other = jnp.where(first, a, b)
                if (1 << k) >= 1024:
                    up = ((g * 1024) >> k) & 1 == 0
                    take_low = first if up else jnp.logical_not(first)
                else:
                    take_low = ((place >> k) ^ (place >> j)) & 1 == 0
                new[v] = jnp.where(take_low, jnp.minimum(x, other), jnp.maximum(x, other))
            parts = new
    stride = mine.shape[0] // tables
    for t in range(tables):
        for g in range(stride // 8):
            at = t * stride + g * 8
            mine[at : at + 8, :] = parts[t * groups + g] if g < groups else jnp.full((8, 128), BIG, jnp.int32)

    for o in range(owners):
        for t in range(tables):
            if o == 0:
                x = mine[t * stride : t * stride + 8, :]
            else:
                off = before[(o - 1) * tables + t, 0]
                low = off & 7

                def columns(first):
                    at = t * stride + ((first >> 7) << 3)
                    left = 128 - (first & 127)
                    turn = left & 127
                    p = pltpu.roll(mine[pl.ds(at, 8), :], turn, 1)
                    q = pltpu.roll(mine[pl.ds(at + 8, 8), :], turn, 1)
                    return pltpu.roll(jnp.where(lane < left, p, q), (8 - low) & 7, 0)

                x = jnp.where(sub < 8 - low, columns(off >> 3), columns((off >> 3) + 1))
            x = x - o * span
            ours = jnp.logical_and(x >= 0, x < span)
            outbox[o, t * 8 : t * 8 + 8, :] = jnp.where(ours, x, span)


    far_first = sorted(range(1, outer), key=lambda d: -min(d, outer - d)) + [0]
    slots = [(dz, d) for dz in far_first for d in [*range(1, inner), 0]]
    pl.semaphore_wait(barrier, len(peers))
    sends, key_in = [], {}
    for k, (dz, d) in enumerate(slots):
        if dz or d:
            to = gx_at(outer - dz, inner - d)
            key_in[k] = remote(outbox.at[to["gx"]], held.at[k], ksend.at[k], krec.at[k], to)
            key_in[k].start()
            sends.append(key_in[k])

    row_copies = {}

    def prepare(k):
        if k in key_in:
            key_in[k].wait_recv()
        for t in range(tables):
            at = pl.ds(t * 8, 8)
            x = held[k, at, :] if k in key_in else outbox[me, at, :]
            row_list[k, :, t : t + 1, :] = ((x & (rows_dev - 1)) + t * rows_dev)[:, None, :]
            bag_list[k, at, :] = x >> log2(rows_dev)
        row_copies[k] = [
            pltpu.make_async_copy(row_list.at[k, u], rows[u].at[pl.ds(k * tables, tables)], rsem.at[k, u])
            for u in range(8)
        ]
        for copy in row_copies[k]:
            copy.start()

    lanes = 2 * bag_size * samples // owners // 8
    if lanes < 128:
        stage[...] = jnp.zeros_like(stage)
    bag_index = lax.broadcasted_iota(jnp.int32, (samples, 128), 0)
    halves = 2
    some = tables // halves

    def pool(k, h, part):
        @pl.loop(0, some * (lanes // 8))
        def _(i):
            local = i // (lanes // 8)
            first = lax.rem(i, lanes // 8) * 8
            line = k * tables + h * some + local
            for q in range(8):
                for u in range(8):
                    row = rows[u][line, first + q]
                    stage[pl.ds(local * 1024 + first + u * 128 + q, 1), :] = tab[pl.ds(row, 1), :]

        for local in range(some):
            t = h * some + local
            picks = []
            for u in range(8):
                bag = bag_list[k, t * 8 + u : t * 8 + u + 1, :]
                picks.append(jnp.where(bag_index == bag, 1.0, 0.0).astype(jnp.bfloat16))
            picked = stage[local * 1024 : local * 1024 + 1024, :].astype(jnp.bfloat16)
            total = jnp.dot(jnp.concatenate(picks, axis=1), picked, preferred_element_type=jnp.float32)
            part[:, t * emb : (t + 1) * emb] = total.astype(part.dtype)

    y_in, z_in = {}, {}

    def along_z(dz, n, at):
        total = part_own[dz, at[0], at[1]].astype(jnp.float32)
        for d in range(1, inner):
            total += from_y[d - 1, dz, at[0], at[1]].astype(jnp.float32)
        sum_y[dz - 1, at[0], at[1]] = total.astype(sum_y.dtype)
        z_in[dz, n] = remote(
            sum_y.at[dz - 1, at[0], at[1]],
            from_z.at[dz - 1, at[0], at[1]],
            zsend.at[dz - 1, n],
            zrec.at[dz - 1, n],
            gx_at(dz, 0),
        )
        z_in[dz, n].start()
        sends.append(z_in[dz, n])

    def half_of(h):
        return pl.ds(h * width // halves, width // halves)

    def chunk_of(q):
        return pl.ds(q * step, step)

    whole = pl.ds(0, width)
    last = far_first[outer - 2]

    def z_event(dz, n):
        if dz == last:
            for h in range(halves):
                for d in range(1, inner):
                    y_in[dz, d, h].wait_recv()
            for q in range(chunks):
                along_z(dz, q, (chunk_of(q), whole))
        else:
            for d in range(1, inner):
                y_in[dz, d, n].wait_recv()
            along_z(dz, n, (pl.ds(0, samples), half_of(n)))

    due = {}
    waits = [(0, 2), (1, 3)]
    for i, dz in enumerate(far_first[: outer - 1]):
        end = (i + 1) * inner * halves
        if dz == last:
            due.setdefault(min(end + 3, len(slots) * halves), []).append((dz, 0))
        else:
            for n in range(halves):
                due.setdefault(min(end + waits[min(i, 1)][n], len(slots) * halves), []).append((dz, n))

    prepare(0)
    prepare(1)
    for load in tables_in:
        load.wait()
    done = 0
    for k, (dz, d) in enumerate(slots):
        if k + 2 < len(slots):
            prepare(k + 2)
        for copy in row_copies[k]:
            copy.wait()
        part = part_y.at[d - 1, dz] if d else part_own.at[dz]
        for h in range(halves):
            pool(k, h, part)
            if d:
                y_in[dz, d, h] = remote(
                    part.at[:, half_of(h)],
                    from_y.at[d - 1, dz, :, half_of(h)],
                    ysend.at[d - 1, dz, h],
                    yrec.at[d - 1, dz, h],
                    gx_at(0, d),
                )
                y_in[dz, d, h].start()
                sends.append(y_in[dz, d, h])
            done += 1
            for event in due.get(done, []):
                z_event(*event)

    far, near = {}, {}
    for d in range(1, inner):
        for h in range(halves):
            y_in[0, d, h].wait_recv()
    for dz in range(1, outer):
        if dz != last:
            for n in range(halves):
                z_in[dz, n].wait_recv()
    for q in range(chunks):
        z_in[last, q].wait_recv()
        at = chunk_of(q)
        total = part_own[0, at, :].astype(jnp.float32)
        for d in range(1, inner):
            total += from_y[d - 1, 0, at, :].astype(jnp.float32)
        for dz in range(1, outer):
            total += from_z[dz - 1, at, :].astype(jnp.float32)
        feat[0, q, 0:step, :] = total.astype(feat.dtype)
        for d in range(1, chips):
            far[d, q] = remote(
                feat.at[0, q, pl.ds(0, step)],
                feat.at[chips - d, q, pl.ds(0, step)],
                gsend.at[d, q],
                grec.at[chips - d, q],
                chip_at(d),
            )
            far[d, q].start()
        near[0, q] = remote(
            feat.at[0, q, pl.ds(0, step)], feat.at[0, q, pl.ds(step, step)], nsend.at[0, q], nrec.at[0, q], partner
        )
        near[0, q].start()

    for load in weights_in:
        load.wait()
    hidden, outs = w_in.shape[1], w_out.shape[1]
    in_tile, out_tile = min(1024, hidden), min(512, outs)
    back, far_out = {}, {}

    def scores(d, q):
        @pl.loop(0, hidden // in_tile)
        def _(i):
            cols = pl.ds(pl.multiple_of(i * in_tile, in_tile), in_tile)
            pre = jnp.dot(feat[d, q], w_in[:, cols], preferred_element_type=jnp.float32) + bias_ref[:, cols]
            hid[:, cols] = jnp.maximum(pre, 0.0).astype(hid.dtype)

        @pl.loop(0, outs // out_tile)
        def _(i):
            cols = pl.ds(pl.multiple_of(i * out_tile, out_tile), out_tile)
            score = jnp.dot(hid[...], w_out[:, cols], preferred_element_type=jnp.float32)
            kept[d, q, :, cols] = score[0:step]
            give[d, q, :, cols] = score[step : 2 * step].astype(give.dtype)

        back[d, q] = remote(give.at[d, q], take.at[d, q], bsend.at[d, q], brec.at[d, q], partner)
        back[d, q].start()

    def forward(d, q):
        far[chips - d, q].wait_recv()
        near[d, q] = remote(
            feat.at[d, q, pl.ds(0, step)], feat.at[d, q, pl.ds(step, step)], nsend.at[d, q], nrec.at[d, q], partner
        )
        near[d, q].start()

    def along_x(d, q):
        back[d, q].wait_recv()
        total = kept[d, q] + take[d, q].astype(jnp.float32)
        x_send[d - 1, q] = total.astype(x_send.dtype)
        far_out[d, q] = remote(
            x_send.at[d - 1, q], x_take.at[d - 1, q], fsend.at[d - 1, q], frec.at[d - 1, q], chip_at(d)
        )
        far_out[d, q].start()

    work = [(d, q) for q in range(chunks) for d in range(1, chips)]
    forward(*work[0])
    near[0, 0].wait_recv()
    scores(0, 0)
    for i, (d, q) in enumerate(work):
        if i + 1 < len(work):
            forward(*work[i + 1])
        near[d, q].wait_recv()
        scores(d, q)
        if i:
            along_x(*work[i - 1])
    rest = list(range(1, chunks))
    near[0, rest[0]].wait_recv()
    along_x(*work[-1])
    for q in rest:
        if q != rest[0]:
            near[0, q].wait_recv()
        scores(0, q)
    for q in range(chunks):
        back[0, q].wait_recv()
        total = kept[0, q] + take[0, q].astype(jnp.float32)
        for d in range(1, chips):
            far_out[d, q].wait_recv()
            total += x_take[d - 1, q].astype(jnp.float32)
        out_ref[chunk_of(q), :] = total.astype(out_ref.dtype)

    for group in (far, near, back, far_out):
        sends += list(group.values())
    for copy in sends:
        copy.wait_send()


def local(table, lookup_owner, lookup_row, bag_length, top_in, top_bias, top_out):
    owners = lax.axis_size("gx")
    tables, samples, bag_size = lookup_row.shape
    rows_dev = table.shape[1]
    emb = table.shape[2]
    count = samples * bag_size
    assert 2 * count // owners <= 1024
    inner = max(1, owners // 4)
    outer = owners // inner
    chips = lax.axis_size("gy") // 2
    width = tables * emb
    hidden, outs = top_out.shape
    step = samples // CHUNKS
    bf16, f32, i32, dma = jnp.bfloat16, jnp.float32, jnp.int32, pltpu.SemaphoreType.DMA
    vmem = pl.BlockSpec(memory_space=pltpu.VMEM)
    anywhere = pl.BlockSpec(memory_space=pl.ANY)
    windows = pltpu.VMEM((owners, tables * 8, 128), i32)
    pieces = max(CHUNKS, 2)
    pairs = [dma((owners,))] * 2 + [dma((inner - 1, outer, 2))] * 2 + [dma((outer - 1, pieces))] * 2
    pairs += [dma((chips, CHUNKS))] * 6 + [dma((chips - 1, CHUNKS))] * 2
    return pl.pallas_call(
        bags_kernel,
        out_shape=jax.ShapeDtypeStruct((samples, outs), bf16),
        in_specs=[vmem, vmem, vmem, anywhere, anywhere, vmem, anywhere],
        out_specs=vmem,
        scratch_shapes=[
            pltpu.VMEM((tables * (count // 128 + 16), 128), i32),
            windows,
            windows,
            pltpu.VMEM((owners, 8, tables, 128), i32),
            windows,
            [pltpu.SMEM((owners * tables, 128), i32) for _ in range(8)],
            pltpu.VMEM((tables * rows_dev, emb), f32),
            pltpu.VMEM((tables // 2 * 1024, emb), f32),
            pltpu.VMEM((inner - 1, outer, samples, width), bf16),
            pltpu.VMEM((outer, samples, width), bf16),
            pltpu.VMEM((inner - 1, outer, samples, width), bf16),
            pltpu.VMEM((outer - 1, samples, width), bf16),
            pltpu.VMEM((outer - 1, samples, width), bf16),
            pltpu.VMEM((chips, CHUNKS, 2 * step, width), bf16),
            pltpu.VMEM((width, hidden), bf16),
            pltpu.VMEM((hidden, outs), bf16),
            pltpu.VMEM((2 * step, hidden), bf16),
            pltpu.VMEM((chips, CHUNKS, step, outs), f32),
            pltpu.VMEM((chips, CHUNKS, step, outs), bf16),
            pltpu.VMEM((chips, CHUNKS, step, outs), bf16),
            pltpu.VMEM((chips - 1, CHUNKS, step, outs), bf16),
            pltpu.VMEM((chips - 1, CHUNKS, step, outs), bf16),
            dma((tables,)),
            dma((2,)),
            dma((owners, 8)),
            *pairs,
        ],
        compiler_params=pltpu.CompilerParams(
            collective_id=0, has_side_effects=True, vmem_limit_bytes=60 * 2**20
        ),
        name="bags",
    )(
        jnp.transpose(lookup_owner[..., 0], (0, 2, 1)),
        jnp.transpose(lookup_row, (0, 2, 1)),
        bag_length,
        table,
        top_in,
        top_bias[None, :],
        top_out,
    )


def solution(mesh):
    return jax.shard_map(
        local,
        mesh=mesh,
        in_specs=(
            P(None, "gx", None),
            P(None, ("gx", "gy"), None, None),
            P(None, ("gx", "gy"), None),
            P(None, ("gx", "gy")),
            P(None, "gy"),
            P("gy"),
            P("gy", None),
        ),
        out_specs=P(("gx", "gy"), None),
        check_vma=False,
    )
```

```python
import jax
import jax.numpy as jnp
from jax import lax
from jax.experimental import pallas as pl
from jax.experimental.pallas import tpu as pltpu
from jax.sharding import PartitionSpec as P

CHUNKS = 4
BIG = 2**31 - 1
MESH = pl.DeviceIdType.MESH


def log2(n):
    return n.bit_length() - 1


def bags_kernel(owner_ref, row_ref, bag_ref, table_ref, top_in_ref, bias_ref, top_out_ref, out_ref, mine, outbox, held, row_list, bag_list, rows, tab, stage, part_y, part_own, from_y, sum_y, from_z, feat, w_in, w_out, hid, kept, give, take, x_send, x_take, tsem, wsem, rsem, ksend, krec, ysend, yrec, zsend, zrec, gsend, grec, nsend, nrec, bsend, brec, fsend, frec):
    owners = held.shape[0]
    inner, outer = from_y.shape[0] + 1, sum_y.shape[0] + 1
    chips, chunks, rows_pair, width = feat.shape
    step = rows_pair // 2
    rows_dev = table_ref.shape[1]
    emb = table_ref.shape[2]
    me, mine_y = lax.axis_index("gx"), lax.axis_index("gy")
    z, y = me // inner, lax.rem(me, inner)
    chip, core = mine_y // 2, lax.rem(mine_y, 2)
    partner = {"gy": chip * 2 + 1 - core}

    def remote(src, dst, send, recv, device):
        return pltpu.make_async_remote_copy(
            src_ref=src, dst_ref=dst, send_sem=send, recv_sem=recv, device_id=device, device_id_type=MESH
        )

    def gx_at(dz, d):
        return {"gx": lax.rem(z + dz, outer) * inner + lax.rem(y + d, inner)}

    def chip_at(d):
        return {"gy": lax.rem(chip + d, chips) * 2 + core}

    barrier = pltpu.get_barrier_semaphore()
    peers = [gx_at(dz, d) for dz in range(outer) for d in range(inner) if dz or d]
    peers += [partner] + [chip_at(d) for d in range(1, chips)]
    for peer in peers:
        pl.semaphore_signal(barrier, inc=1, device_id=peer, device_id_type=MESH)
    tables_in = [
        pltpu.make_async_copy(table_ref.at[t], tab[t], tsem.at[t])
        for t in range(table_ref.shape[0])
    ]
    weights_in = [
        pltpu.make_async_copy(top_in_ref, w_in, wsem.at[0]),
        pltpu.make_async_copy(top_out_ref, w_out, wsem.at[1]),
    ]
    for load in tables_in + weights_in:
        load.start()

    tables, bag_size, samples = row_ref.shape
    owner = owner_ref[:, :, 0, :]
    slot = lax.broadcasted_iota(jnp.int32, owner.shape, 1)
    sample = lax.broadcasted_iota(jnp.int32, owner.shape, 2)
    live = slot < bag_ref[...][:, None, :]
    key = jnp.where(live, (owner * samples + sample) * rows_dev + row_ref[...], BIG)
    count = bag_size * samples
    groups = count // 1024
    parts = []
    for t in range(tables):
        for c in range(samples // 128):
            for r in range(bag_size // 8):
                parts.append(key[t, r * 8 : r * 8 + 8, c * 128 : c * 128 + 128])
    lane = lax.broadcasted_iota(jnp.int32, (8, 128), 1)
    sub = lax.broadcasted_iota(jnp.int32, (8, 128), 0)
    place = lane * 8 + sub
    bits = log2(count)
    span = samples * rows_dev

    before = []
    for o in range(1, owners):
        for t in range(tables):
            tally = jnp.zeros((8, 128), jnp.int32)
            for g in range(groups):
                tally += (parts[t * groups + g] < o * span).astype(jnp.int32)
            before.append(jnp.sum(tally, axis=0, keepdims=True))
    before = jnp.sum(jnp.concatenate(before, axis=0), axis=1, keepdims=True)

    for k in range(1, bits + 1):
        for j in range(k - 1, -1, -1):
            d = 1 << j
            new = [None] * len(parts)
            for v in range(len(parts)):
                g = v % groups
                if d >= 1024:
                    gd = d // 1024
                    if g & gd:
                        continue
                    w = v + gd
                    low = jnp.minimum(parts[v], parts[w])
                    high = jnp.maximum(parts[v], parts[w])
                    up = ((g * 1024) >> k) & 1 == 0
                    new[v], new[w] = (low, high) if up else (high, low)
                    continue
                x = parts[v]
                if d < 8:
                    a, b = pltpu.roll(x, 8 - d, 0), pltpu.roll(x, d, 0)
                else:
                    s = d // 8
                    a, b = pltpu.roll(x, 128 - s, 1), pltpu.roll(x, s, 1)
                first = (place & d) == 0
                other = jnp.where(first, a, b)
                if (1 << k) >= 1024:
                    up = ((g * 1024) >> k) & 1 == 0
                    take_low = first if up else jnp.logical_not(first)
                else:
                    take_low = ((place >> k) ^ (place >> j)) & 1 == 0
                new[v] = jnp.where(take_low, jnp.minimum(x, other), jnp.maximum(x, other))
            parts = new
    stride = mine.shape[0] // tables
    for t in range(tables):
        for g in range(stride // 8):
            at = t * stride + g * 8
            mine[at : at + 8, :] = parts[t * groups + g] if g < groups else jnp.full((8, 128), BIG, jnp.int32)

    for o in range(owners):
        for t in range(tables):
            if o == 0:
                x = mine[t * stride : t * stride + 8, :]
            else:
                off = before[(o - 1) * tables + t, 0]
                low = off & 7

                def columns(first):
                    at = t * stride + ((first >> 7) << 3)
                    left = 128 - (first & 127)
                    turn = left & 127
                    p = pltpu.roll(mine[pl.ds(at, 8), :], turn, 1)
                    q = pltpu.roll(mine[pl.ds(at + 8, 8), :], turn, 1)
                    return pltpu.roll(jnp.where(lane < left, p, q), (8 - low) & 7, 0)

                x = jnp.where(sub < 8 - low, columns(off >> 3), columns((off >> 3) + 1))
            x = x - o * span
            ours = jnp.logical_and(x >= 0, x < span)
            outbox[o, t * 8 : t * 8 + 8, :] = jnp.where(ours, x, span)


    far_first = sorted(range(1, outer), key=lambda d: -min(d, outer - d)) + [0]
    slots = [(dz, d) for dz in far_first for d in [*range(1, inner), 0]]
    pl.semaphore_wait(barrier, len(peers))
    sends, key_in = [], {}
    for k, (dz, d) in enumerate(slots):
        if dz or d:
            to = gx_at(outer - dz, inner - d)
            key_in[k] = remote(outbox.at[to["gx"]], held.at[k], ksend.at[k], krec.at[k], to)
            key_in[k].start()
            sends.append(key_in[k])

    row_copies = {}

    def prepare(k):
        if k in key_in:
            key_in[k].wait_recv()
        for t in range(tables):
            at = pl.ds(t * 8, 8)
            x = held[k, at, :] if k in key_in else outbox[me, at, :]
            row_list[k, :, t : t + 1, :] = (x & (rows_dev - 1))[:, None, :]
            bag_list[k, at, :] = x >> log2(rows_dev)
        row_copies[k] = [
            pltpu.make_async_copy(row_list.at[k, u], rows[u].at[pl.ds(k * tables, tables)], rsem.at[k, u])
            for u in range(8)
        ]
        for copy in row_copies[k]:
            copy.start()

    lanes = 2 * bag_size * samples // owners // 8
    if lanes < 128:
        stage[...] = jnp.zeros_like(stage)
    bag_index = lax.broadcasted_iota(jnp.int32, (samples, 128), 0)
    halves = 2
    some = tables // halves

    def pool(k, h, part):
        for local in range(some):
            t = h * some + local
            line = k * tables + t
            lists = [rows[u].at[line] for u in range(8)]

            @pl.loop(0, lanes // 8)
            def _(i):
                for q in range(8):
                    for u in range(8):
                        row = lists[u][i * 8 + q]
                        stage[pl.ds(local * 1024 + i * 8 + u * 128 + q, 1), :] = tab[t][pl.ds(row, 1), :]

        for local in range(some):
            t = h * some + local
            picks = []
            for u in range(8):
                bag = bag_list[k, t * 8 + u : t * 8 + u + 1, :]
                picks.append(jnp.where(bag_index == bag, 1.0, 0.0).astype(jnp.bfloat16))
            picked = stage[local * 1024 : local * 1024 + 1024, :].astype(jnp.bfloat16)
            total = jnp.dot(jnp.concatenate(picks, axis=1), picked, preferred_element_type=jnp.float32)
            part[:, t * emb : (t + 1) * emb] = total.astype(part.dtype)

    y_in, z_in = {}, {}

    def along_z(dz, n, at):
        total = part_own[dz, at[0], at[1]].astype(jnp.float32)
        for d in range(1, inner):
            total += from_y[d - 1, dz, at[0], at[1]].astype(jnp.float32)
        sum_y[dz - 1, at[0], at[1]] = total.astype(sum_y.dtype)
        z_in[dz, n] = remote(
            sum_y.at[dz - 1, at[0], at[1]],
            from_z.at[dz - 1, at[0], at[1]],
            zsend.at[dz - 1, n],
            zrec.at[dz - 1, n],
            gx_at(dz, 0),
        )
        z_in[dz, n].start()
        sends.append(z_in[dz, n])

    def half_of(h):
        return pl.ds(h * width // halves, width // halves)

    def chunk_of(q):
        return pl.ds(q * step, step)

    whole = pl.ds(0, width)
    last = far_first[outer - 2]

    def z_event(dz, n):
        if dz == last:
            for h in range(halves):
                for d in range(1, inner):
                    y_in[dz, d, h].wait_recv()
            for q in range(chunks):
                along_z(dz, q, (chunk_of(q), whole))
        else:
            for d in range(1, inner):
                y_in[dz, d, n].wait_recv()
            along_z(dz, n, (pl.ds(0, samples), half_of(n)))

    due = {}
    waits = [(0, 2), (1, 3)]
    for i, dz in enumerate(far_first[: outer - 1]):
        end = (i + 1) * inner * halves
        if dz == last:
            due.setdefault(min(end + 3, len(slots) * halves), []).append((dz, 0))
        else:
            for n in range(halves):
                due.setdefault(min(end + waits[min(i, 1)][n], len(slots) * halves), []).append((dz, n))

    prepare(0)
    prepare(1)
    done = 0
    for k, (dz, d) in enumerate(slots):
        if k + 2 < len(slots):
            prepare(k + 2)
        for copy in row_copies[k]:
            copy.wait()
        part = part_y.at[d - 1, dz] if d else part_own.at[dz]
        for h in range(halves):
            if k == 0:
                for t in range(h * some, (h + 1) * some):
                    tables_in[t].wait()
            pool(k, h, part)
            if d:
                y_in[dz, d, h] = remote(
                    part.at[:, half_of(h)],
                    from_y.at[d - 1, dz, :, half_of(h)],
                    ysend.at[d - 1, dz, h],
                    yrec.at[d - 1, dz, h],
                    gx_at(0, d),
                )
                y_in[dz, d, h].start()
                sends.append(y_in[dz, d, h])
            done += 1
            for event in due.get(done, []):
                z_event(*event)

    far, near = {}, {}
    for d in range(1, inner):
        for h in range(halves):
            y_in[0, d, h].wait_recv()
    for dz in range(1, outer):
        if dz != last:
            for n in range(halves):
                z_in[dz, n].wait_recv()
    for q in range(chunks):
        z_in[last, q].wait_recv()
        at = chunk_of(q)
        total = part_own[0, at, :].astype(jnp.float32)
        for d in range(1, inner):
            total += from_y[d - 1, 0, at, :].astype(jnp.float32)
        for dz in range(1, outer):
            total += from_z[dz - 1, at, :].astype(jnp.float32)
        feat[0, q, 0:step, :] = total.astype(feat.dtype)
        for d in range(1, chips):
            far[d, q] = remote(
                feat.at[0, q, pl.ds(0, step)],
                feat.at[chips - d, q, pl.ds(0, step)],
                gsend.at[d, q],
                grec.at[chips - d, q],
                chip_at(d),
            )
            far[d, q].start()
        near[0, q] = remote(
            feat.at[0, q, pl.ds(0, step)], feat.at[0, q, pl.ds(step, step)], nsend.at[0, q], nrec.at[0, q], partner
        )
        near[0, q].start()

    for load in weights_in:
        load.wait()
    hidden, outs = w_in.shape[1], w_out.shape[1]
    in_tile, out_tile = min(1024, hidden), min(512, outs)
    back, far_out = {}, {}

    def scores(d, q):
        @pl.loop(0, hidden // in_tile)
        def _(i):
            cols = pl.ds(pl.multiple_of(i * in_tile, in_tile), in_tile)
            pre = jnp.dot(feat[d, q], w_in[:, cols], preferred_element_type=jnp.float32) + bias_ref[:, cols]
            hid[:, cols] = jnp.maximum(pre, 0.0).astype(hid.dtype)

        @pl.loop(0, outs // out_tile)
        def _(i):
            cols = pl.ds(pl.multiple_of(i * out_tile, out_tile), out_tile)
            score = jnp.dot(hid[...], w_out[:, cols], preferred_element_type=jnp.float32)
            kept[d, q, :, cols] = score[0:step]
            give[d, q, :, cols] = score[step : 2 * step].astype(give.dtype)

        back[d, q] = remote(give.at[d, q], take.at[d, q], bsend.at[d, q], brec.at[d, q], partner)
        back[d, q].start()

    def forward(d, q):
        far[chips - d, q].wait_recv()
        near[d, q] = remote(
            feat.at[d, q, pl.ds(0, step)], feat.at[d, q, pl.ds(step, step)], nsend.at[d, q], nrec.at[d, q], partner
        )
        near[d, q].start()

    def along_x(d, q):
        back[d, q].wait_recv()
        total = kept[d, q] + take[d, q].astype(jnp.float32)
        x_send[d - 1, q] = total.astype(x_send.dtype)
        far_out[d, q] = remote(
            x_send.at[d - 1, q], x_take.at[d - 1, q], fsend.at[d - 1, q], frec.at[d - 1, q], chip_at(d)
        )
        far_out[d, q].start()

    work = [(d, q) for q in range(chunks) for d in range(1, chips)]
    forward(*work[0])
    near[0, 0].wait_recv()
    scores(0, 0)
    for i, (d, q) in enumerate(work):
        if i + 1 < len(work):
            forward(*work[i + 1])
        near[d, q].wait_recv()
        scores(d, q)
        if i:
            along_x(*work[i - 1])
    rest = list(range(1, chunks))
    near[0, rest[0]].wait_recv()
    along_x(*work[-1])
    for q in rest:
        if q != rest[0]:
            near[0, q].wait_recv()
        scores(0, q)
    for q in range(chunks):
        back[0, q].wait_recv()
        total = kept[0, q] + take[0, q].astype(jnp.float32)
        for d in range(1, chips):
            far_out[d, q].wait_recv()
            total += x_take[d - 1, q].astype(jnp.float32)
        out_ref[chunk_of(q), :] = total.astype(out_ref.dtype)

    for group in (far, near, back, far_out):
        sends += list(group.values())
    for copy in sends:
        copy.wait_send()


def local(table, lookup_owner, lookup_row, bag_length, top_in, top_bias, top_out):
    owners = lax.axis_size("gx")
    tables, samples, bag_size = lookup_row.shape
    rows_dev = table.shape[1]
    emb = table.shape[2]
    count = samples * bag_size
    assert 2 * count // owners <= 1024
    inner = max(1, owners // 4)
    outer = owners // inner
    chips = lax.axis_size("gy") // 2
    width = tables * emb
    hidden, outs = top_out.shape
    step = samples // CHUNKS
    bf16, f32, i32, dma = jnp.bfloat16, jnp.float32, jnp.int32, pltpu.SemaphoreType.DMA
    vmem = pl.BlockSpec(memory_space=pltpu.VMEM)
    anywhere = pl.BlockSpec(memory_space=pl.ANY)
    windows = pltpu.VMEM((owners, tables * 8, 128), i32)
    pieces = max(CHUNKS, 2)
    pairs = [dma((owners,))] * 2 + [dma((inner - 1, outer, 2))] * 2 + [dma((outer - 1, pieces))] * 2
    pairs += [dma((chips, CHUNKS))] * 6 + [dma((chips - 1, CHUNKS))] * 2
    return pl.pallas_call(
        bags_kernel,
        out_shape=jax.ShapeDtypeStruct((samples, outs), bf16),
        in_specs=[vmem, vmem, vmem, anywhere, anywhere, vmem, anywhere],
        out_specs=vmem,
        scratch_shapes=[
            pltpu.VMEM((tables * (count // 128 + 16), 128), i32),
            windows,
            windows,
            pltpu.VMEM((owners, 8, tables, 128), i32),
            windows,
            [pltpu.SMEM((owners * tables, 128), i32) for _ in range(8)],
            [pltpu.VMEM((rows_dev, emb), f32) for _ in range(tables)],
            pltpu.VMEM((tables // 2 * 1024, emb), f32),
            pltpu.VMEM((inner - 1, outer, samples, width), bf16),
            pltpu.VMEM((outer, samples, width), bf16),
            pltpu.VMEM((inner - 1, outer, samples, width), bf16),
            pltpu.VMEM((outer - 1, samples, width), bf16),
            pltpu.VMEM((outer - 1, samples, width), bf16),
            pltpu.VMEM((chips, CHUNKS, 2 * step, width), bf16),
            pltpu.VMEM((width, hidden), bf16),
            pltpu.VMEM((hidden, outs), bf16),
            pltpu.VMEM((2 * step, hidden), bf16),
            pltpu.VMEM((chips, CHUNKS, step, outs), f32),
            pltpu.VMEM((chips, CHUNKS, step, outs), bf16),
            pltpu.VMEM((chips, CHUNKS, step, outs), bf16),
            pltpu.VMEM((chips - 1, CHUNKS, step, outs), bf16),
            pltpu.VMEM((chips - 1, CHUNKS, step, outs), bf16),
            dma((tables,)),
            dma((2,)),
            dma((owners, 8)),
            *pairs,
        ],
        compiler_params=pltpu.CompilerParams(
            collective_id=0, has_side_effects=True, vmem_limit_bytes=60 * 2**20
        ),
        name="bags",
    )(
        jnp.transpose(lookup_owner, (0, 2, 3, 1)),
        jnp.transpose(lookup_row, (0, 2, 1)),
        bag_length,
        table,
        top_in,
        top_bias[None, :],
        top_out,
    )


def solution(mesh):
    return jax.shard_map(
        local,
        mesh=mesh,
        in_specs=(
            P(None, "gx", None),
            P(None, ("gx", "gy"), None, None),
            P(None, ("gx", "gy"), None),
            P(None, ("gx", "gy")),
            P(None, "gy"),
            P("gy"),
            P("gy", None),
        ),
        out_specs=P(("gx", "gy"), None),
        check_vma=False,
    )
```

```python
import jax
import jax.numpy as jnp
from jax import lax
from jax.experimental import pallas as pl
from jax.experimental.pallas import tpu as pltpu
from jax.sharding import PartitionSpec as P

CHUNKS = 4
BIG = 2**31 - 1
MESH = pl.DeviceIdType.MESH


def log2(n):
    return n.bit_length() - 1


def bags_kernel(owner_ref, row_ref, bag_ref, table_ref, top_in_ref, bias_ref, top_out_ref, out_ref, mine, outbox, held, row_list, bag_list, rows, tab, stage, part_y, part_own, from_y, sum_y, from_z, feat, w_in, w_out, hid, kept, give, take, x_send, x_take, tsem, wsem, rsem, ksend, krec, ysend, yrec, zsend, zrec, gsend, grec, nsend, nrec, bsend, brec, fsend, frec):
    owners = held.shape[0]
    inner, outer = from_y.shape[0] + 1, sum_y.shape[0] + 1
    chips, chunks, rows_pair, width = feat.shape
    step = rows_pair // 2
    rows_dev = table_ref.shape[1]
    emb = table_ref.shape[2]
    me, mine_y = lax.axis_index("gx"), lax.axis_index("gy")
    z, y = me // inner, lax.rem(me, inner)
    chip, core = mine_y // 2, lax.rem(mine_y, 2)
    partner = {"gy": chip * 2 + 1 - core}

    def remote(src, dst, send, recv, device):
        return pltpu.make_async_remote_copy(
            src_ref=src, dst_ref=dst, send_sem=send, recv_sem=recv, device_id=device, device_id_type=MESH
        )

    def gx_at(dz, d):
        return {"gx": lax.rem(z + dz, outer) * inner + lax.rem(y + d, inner)}

    def chip_at(d):
        return {"gy": lax.rem(chip + d, chips) * 2 + core}

    barrier = pltpu.get_barrier_semaphore()
    peers = [gx_at(dz, d) for dz in range(outer) for d in range(inner) if dz or d]
    peers += [partner] + [chip_at(d) for d in range(1, chips)]
    for peer in peers:
        pl.semaphore_signal(barrier, inc=1, device_id=peer, device_id_type=MESH)
    tables_in = [
        pltpu.make_async_copy(table_ref.at[t], tab[t], tsem.at[t])
        for t in range(table_ref.shape[0])
    ]
    weights_in = [
        pltpu.make_async_copy(top_in_ref, w_in, wsem.at[0]),
        pltpu.make_async_copy(top_out_ref, w_out, wsem.at[1]),
    ]
    for load in tables_in + weights_in:
        load.start()

    tables, bag_size, samples = row_ref.shape
    owner = owner_ref[:, :, 0, :]
    slot = lax.broadcasted_iota(jnp.int32, owner.shape, 1)
    sample = lax.broadcasted_iota(jnp.int32, owner.shape, 2)
    live = slot < bag_ref[...][:, None, :]
    key = jnp.where(live, (owner * samples + sample) * rows_dev + row_ref[...], BIG)
    count = bag_size * samples
    groups = count // 1024
    parts = []
    for t in range(tables):
        for c in range(samples // 128):
            for r in range(bag_size // 8):
                parts.append(key[t, r * 8 : r * 8 + 8, c * 128 : c * 128 + 128])
    lane = lax.broadcasted_iota(jnp.int32, (8, 128), 1)
    sub = lax.broadcasted_iota(jnp.int32, (8, 128), 0)
    place = lane * 8 + sub
    bits = log2(count)
    span = samples * rows_dev

    before = []
    for o in range(1, owners):
        for t in range(tables):
            tally = jnp.zeros((8, 128), jnp.int32)
            for g in range(groups):
                tally += (parts[t * groups + g] < o * span).astype(jnp.int32)
            before.append(jnp.sum(tally, axis=0, keepdims=True))
    before = jnp.sum(jnp.concatenate(before, axis=0), axis=1, keepdims=True)

    for k in range(1, bits + 1):
        for j in range(k - 1, -1, -1):
            d = 1 << j
            new = [None] * len(parts)
            for v in range(len(parts)):
                g = v % groups
                if d >= 1024:
                    gd = d // 1024
                    if g & gd:
                        continue
                    w = v + gd
                    low = jnp.minimum(parts[v], parts[w])
                    high = jnp.maximum(parts[v], parts[w])
                    up = ((g * 1024) >> k) & 1 == 0
                    new[v], new[w] = (low, high) if up else (high, low)
                    continue
                x = parts[v]
                if d < 8:
                    a, b = pltpu.roll(x, 8 - d, 0), pltpu.roll(x, d, 0)
                else:
                    s = d // 8
                    a, b = pltpu.roll(x, 128 - s, 1), pltpu.roll(x, s, 1)
                first = (place & d) == 0
                other = jnp.where(first, a, b)
                if (1 << k) >= 1024:
                    up = ((g * 1024) >> k) & 1 == 0
                    take_low = first if up else jnp.logical_not(first)
                else:
                    take_low = ((place >> k) ^ (place >> j)) & 1 == 0
                new[v] = jnp.where(take_low, jnp.minimum(x, other), jnp.maximum(x, other))
            parts = new
    stride = mine.shape[0] // tables
    for t in range(tables):
        for g in range(stride // 8):
            at = t * stride + g * 8
            mine[at : at + 8, :] = parts[t * groups + g] if g < groups else jnp.full((8, 128), BIG, jnp.int32)

    for o in range(owners):
        for t in range(tables):
            if o == 0:
                x = mine[t * stride : t * stride + 8, :]
            else:
                off = before[(o - 1) * tables + t, 0]
                low = off & 7

                def columns(first):
                    at = t * stride + ((first >> 7) << 3)
                    left = 128 - (first & 127)
                    turn = left & 127
                    p = pltpu.roll(mine[pl.ds(at, 8), :], turn, 1)
                    q = pltpu.roll(mine[pl.ds(at + 8, 8), :], turn, 1)
                    return pltpu.roll(jnp.where(lane < left, p, q), (8 - low) & 7, 0)

                x = jnp.where(sub < 8 - low, columns(off >> 3), columns((off >> 3) + 1))
            x = x - o * span
            ours = jnp.logical_and(x >= 0, x < span)
            outbox[o, t * 8 : t * 8 + 8, :] = jnp.where(ours, x, span)


    far_first = sorted(range(1, outer), key=lambda d: -min(d, outer - d)) + [0]
    slots = [(dz, d) for dz in far_first for d in [*range(1, inner), 0]]
    pl.semaphore_wait(barrier, len(peers))
    sends, key_in = [], {}
    for k, (dz, d) in enumerate(slots):
        if dz or d:
            to = gx_at(outer - dz, inner - d)
            key_in[k] = remote(outbox.at[to["gx"]], held.at[k], ksend.at[k], krec.at[k], to)
            key_in[k].start()
            sends.append(key_in[k])

    row_copies = {}

    def prepare(k):
        if k in key_in:
            key_in[k].wait_recv()
        for t in range(tables):
            at = pl.ds(t * 8, 8)
            x = held[k, at, :] if k in key_in else outbox[me, at, :]
            row_list[k, :, t : t + 1, :] = (x & (rows_dev - 1))[:, None, :]
            bag_list[k, at, :] = x >> log2(rows_dev)
        row_copies[k] = [
            pltpu.make_async_copy(row_list.at[k, u], rows[u].at[pl.ds(k * tables, tables)], rsem.at[k, u])
            for u in range(8)
        ]
        for copy in row_copies[k]:
            copy.start()

    lanes = 2 * bag_size * samples // owners // 8
    if lanes < 128:
        stage[...] = jnp.zeros_like(stage)
    bag_index = lax.broadcasted_iota(jnp.int32, (samples, 128), 0)
    halves = 2
    some = tables // halves

    def pool(k, h, part):
        for local in range(some):
            t = h * some + local
            line = k * tables + t
            lists = [rows[u].at[line] for u in range(8)]

            @pl.loop(0, lanes // 16)
            def _(i):
                for q in range(16):
                    for u in range(8):
                        row = lists[u][i * 16 + q]
                        stage[pl.ds(local * 1024 + i * 16 + u * 128 + q, 1), :] = tab[t][pl.ds(row, 1), :]

        for local in range(some):
            t = h * some + local
            picks = []
            for u in range(8):
                bag = bag_list[k, t * 8 + u : t * 8 + u + 1, :]
                picks.append(jnp.where(bag_index == bag, 1.0, 0.0).astype(jnp.bfloat16))
            picked = stage[local * 1024 : local * 1024 + 1024, :].astype(jnp.bfloat16)
            total = jnp.dot(jnp.concatenate(picks, axis=1), picked, preferred_element_type=jnp.float32)
            part[:, t * emb : (t + 1) * emb] = total.astype(part.dtype)

    y_in, z_in = {}, {}

    def along_z(dz, n, at):
        total = part_own[dz, at[0], at[1]].astype(jnp.float32)
        for d in range(1, inner):
            total += from_y[d - 1, dz, at[0], at[1]].astype(jnp.float32)
        sum_y[dz - 1, at[0], at[1]] = total.astype(sum_y.dtype)
        z_in[dz, n] = remote(
            sum_y.at[dz - 1, at[0], at[1]],
            from_z.at[dz - 1, at[0], at[1]],
            zsend.at[dz - 1, n],
            zrec.at[dz - 1, n],
            gx_at(dz, 0),
        )
        z_in[dz, n].start()
        sends.append(z_in[dz, n])

    def half_of(h):
        return pl.ds(h * width // halves, width // halves)

    def chunk_of(q):
        return pl.ds(q * step, step)

    whole = pl.ds(0, width)
    last = far_first[outer - 2]

    def z_event(dz, n):
        if dz == last:
            for h in range(halves):
                for d in range(1, inner):
                    y_in[dz, d, h].wait_recv()
            for q in range(chunks):
                along_z(dz, q, (chunk_of(q), whole))
        else:
            for d in range(1, inner):
                y_in[dz, d, n].wait_recv()
            along_z(dz, n, (pl.ds(0, samples), half_of(n)))

    due = {}
    waits = [(0, 2), (1, 3)]
    for i, dz in enumerate(far_first[: outer - 1]):
        end = (i + 1) * inner * halves
        if dz == last:
            due.setdefault(min(end + 3, len(slots) * halves), []).append((dz, 0))
        else:
            for n in range(halves):
                due.setdefault(min(end + waits[min(i, 1)][n], len(slots) * halves), []).append((dz, n))

    prepare(0)
    prepare(1)
    done = 0
    for k, (dz, d) in enumerate(slots):
        if k + 2 < len(slots):
            prepare(k + 2)
        for copy in row_copies[k]:
            copy.wait()
        part = part_y.at[d - 1, dz] if d else part_own.at[dz]
        for h in range(halves):
            if k == 0:
                for t in range(h * some, (h + 1) * some):
                    tables_in[t].wait()
            pool(k, h, part)
            if d:
                y_in[dz, d, h] = remote(
                    part.at[:, half_of(h)],
                    from_y.at[d - 1, dz, :, half_of(h)],
                    ysend.at[d - 1, dz, h],
                    yrec.at[d - 1, dz, h],
                    gx_at(0, d),
                )
                y_in[dz, d, h].start()
                sends.append(y_in[dz, d, h])
            done += 1
            for event in due.get(done, []):
                z_event(*event)

    far, near = {}, {}
    for d in range(1, inner):
        for h in range(halves):
            y_in[0, d, h].wait_recv()
    for dz in range(1, outer):
        if dz != last:
            for n in range(halves):
                z_in[dz, n].wait_recv()
    for q in range(chunks):
        z_in[last, q].wait_recv()
        at = chunk_of(q)
        total = part_own[0, at, :].astype(jnp.float32)
        for d in range(1, inner):
            total += from_y[d - 1, 0, at, :].astype(jnp.float32)
        for dz in range(1, outer):
            total += from_z[dz - 1, at, :].astype(jnp.float32)
        feat[0, q, 0:step, :] = total.astype(feat.dtype)
        for d in range(1, chips):
            far[d, q] = remote(
                feat.at[0, q, pl.ds(0, step)],
                feat.at[chips - d, q, pl.ds(0, step)],
                gsend.at[d, q],
                grec.at[chips - d, q],
                chip_at(d),
            )
            far[d, q].start()
        near[0, q] = remote(
            feat.at[0, q, pl.ds(0, step)], feat.at[0, q, pl.ds(step, step)], nsend.at[0, q], nrec.at[0, q], partner
        )
        near[0, q].start()

    for load in weights_in:
        load.wait()
    hidden, outs = w_in.shape[1], w_out.shape[1]
    in_tile, out_tile = min(1024, hidden), min(512, outs)
    back, far_out = {}, {}

    def scores(d, q):
        @pl.loop(0, hidden // in_tile)
        def _(i):
            cols = pl.ds(pl.multiple_of(i * in_tile, in_tile), in_tile)
            pre = jnp.dot(feat[d, q], w_in[:, cols], preferred_element_type=jnp.float32) + bias_ref[:, cols]
            hid[:, cols] = jnp.maximum(pre, 0.0).astype(hid.dtype)

        @pl.loop(0, outs // out_tile)
        def _(i):
            cols = pl.ds(pl.multiple_of(i * out_tile, out_tile), out_tile)
            score = jnp.dot(hid[...], w_out[:, cols], preferred_element_type=jnp.float32)
            kept[d, q, :, cols] = score[0:step]
            give[d, q, :, cols] = score[step : 2 * step].astype(give.dtype)

        back[d, q] = remote(give.at[d, q], take.at[d, q], bsend.at[d, q], brec.at[d, q], partner)
        back[d, q].start()

    def forward(d, q):
        far[chips - d, q].wait_recv()
        near[d, q] = remote(
            feat.at[d, q, pl.ds(0, step)], feat.at[d, q, pl.ds(step, step)], nsend.at[d, q], nrec.at[d, q], partner
        )
        near[d, q].start()

    def along_x(d, q):
        back[d, q].wait_recv()
        total = kept[d, q] + take[d, q].astype(jnp.float32)
        x_send[d - 1, q] = total.astype(x_send.dtype)
        far_out[d, q] = remote(
            x_send.at[d - 1, q], x_take.at[d - 1, q], fsend.at[d - 1, q], frec.at[d - 1, q], chip_at(d)
        )
        far_out[d, q].start()

    work = [(d, q) for q in range(chunks) for d in range(1, chips)]
    forward(*work[0])
    near[0, 0].wait_recv()
    scores(0, 0)
    for i, (d, q) in enumerate(work):
        if i + 1 < len(work):
            forward(*work[i + 1])
        near[d, q].wait_recv()
        scores(d, q)
        if i:
            along_x(*work[i - 1])
    rest = list(range(1, chunks))
    near[0, rest[0]].wait_recv()
    along_x(*work[-1])
    for q in rest:
        if q != rest[0]:
            near[0, q].wait_recv()
        scores(0, q)
    for q in range(chunks):
        back[0, q].wait_recv()
        total = kept[0, q] + take[0, q].astype(jnp.float32)
        for d in range(1, chips):
            far_out[d, q].wait_recv()
            total += x_take[d - 1, q].astype(jnp.float32)
        out_ref[chunk_of(q), :] = total.astype(out_ref.dtype)

    for group in (far, near, back, far_out):
        sends += list(group.values())
    for copy in sends:
        copy.wait_send()


def local(table, lookup_owner, lookup_row, bag_length, top_in, top_bias, top_out):
    owners = lax.axis_size("gx")
    tables, samples, bag_size = lookup_row.shape
    rows_dev = table.shape[1]
    emb = table.shape[2]
    count = samples * bag_size
    assert 2 * count // owners <= 1024
    inner = max(1, owners // 4)
    outer = owners // inner
    chips = lax.axis_size("gy") // 2
    width = tables * emb
    hidden, outs = top_out.shape
    step = samples // CHUNKS
    bf16, f32, i32, dma = jnp.bfloat16, jnp.float32, jnp.int32, pltpu.SemaphoreType.DMA
    vmem = pl.BlockSpec(memory_space=pltpu.VMEM)
    anywhere = pl.BlockSpec(memory_space=pl.ANY)
    windows = pltpu.VMEM((owners, tables * 8, 128), i32)
    pieces = max(CHUNKS, 2)
    pairs = [dma((owners,))] * 2 + [dma((inner - 1, outer, 2))] * 2 + [dma((outer - 1, pieces))] * 2
    pairs += [dma((chips, CHUNKS))] * 6 + [dma((chips - 1, CHUNKS))] * 2
    return pl.pallas_call(
        bags_kernel,
        out_shape=jax.ShapeDtypeStruct((samples, outs), bf16),
        in_specs=[vmem, vmem, vmem, anywhere, anywhere, vmem, anywhere],
        out_specs=vmem,
        scratch_shapes=[
            pltpu.VMEM((tables * (count // 128 + 16), 128), i32),
            windows,
            windows,
            pltpu.VMEM((owners, 8, tables, 128), i32),
            windows,
            [pltpu.SMEM((owners * tables, 128), i32) for _ in range(8)],
            [pltpu.VMEM((rows_dev, emb), f32) for _ in range(tables)],
            pltpu.VMEM((tables // 2 * 1024, emb), f32),
            pltpu.VMEM((inner - 1, outer, samples, width), bf16),
            pltpu.VMEM((outer, samples, width), bf16),
            pltpu.VMEM((inner - 1, outer, samples, width), bf16),
            pltpu.VMEM((outer - 1, samples, width), bf16),
            pltpu.VMEM((outer - 1, samples, width), bf16),
            pltpu.VMEM((chips, CHUNKS, 2 * step, width), bf16),
            pltpu.VMEM((width, hidden), bf16),
            pltpu.VMEM((hidden, outs), bf16),
            pltpu.VMEM((2 * step, hidden), bf16),
            pltpu.VMEM((chips, CHUNKS, step, outs), f32),
            pltpu.VMEM((chips, CHUNKS, step, outs), bf16),
            pltpu.VMEM((chips, CHUNKS, step, outs), bf16),
            pltpu.VMEM((chips - 1, CHUNKS, step, outs), bf16),
            pltpu.VMEM((chips - 1, CHUNKS, step, outs), bf16),
            dma((tables,)),
            dma((2,)),
            dma((owners, 8)),
            *pairs,
        ],
        compiler_params=pltpu.CompilerParams(
            collective_id=0, has_side_effects=True, vmem_limit_bytes=60 * 2**20
        ),
        name="bags",
    )(
        jnp.transpose(lookup_owner, (0, 2, 3, 1)),
        jnp.transpose(lookup_row, (0, 2, 1)),
        bag_length,
        table,
        top_in,
        top_bias[None, :],
        top_out,
    )


def solution(mesh):
    return jax.shard_map(
        local,
        mesh=mesh,
        in_specs=(
            P(None, "gx", None),
            P(None, ("gx", "gy"), None, None),
            P(None, ("gx", "gy"), None),
            P(None, ("gx", "gy")),
            P(None, "gy"),
            P("gy"),
            P("gy", None),
        ),
        out_specs=P(("gx", "gy"), None),
        check_vma=False,
    )
```
